32 devices in a mesh: rep: 2 (over x), dp: 16 (over y, z, core).
Axes of the slice: x: 2, y: 2, z: 4, core: 2. Of those that a mesh axis runs over, the one named last changes fastest.
Arguments:
- x: bfloat16 [32, 2048, 640], P(('rep', 'dp')), parts along dimension 0
- dy: bfloat16 [32, 2048, 640], P(('rep', 'dp')), parts along dimension 0
- w_gate: bfloat16 [2, 640, 2560], replicated
- w_up: bfloat16 [2, 640, 2560], replicated
- w_down: bfloat16 [2, 2560, 640], replicated
- m_w_gate: float32 [2, 640, 2560], P(None, 'dp')
- m_w_up: float32 [2, 640, 2560], P(None, 'dp')
- m_w_down: float32 [2, 2560, 640], P(None, 'dp')
- v_w_gate: float32 [2, 640, 2560], P(None, 'dp')
- v_w_up: float32 [2, 640, 2560], P(None, 'dp')
- v_w_down: float32 [2, 2560, 640], P(None, 'dp')
Outputs:
- output 1: bfloat16 [4, 640, 2560], P('rep'), parts along dimension 0
- output 2: bfloat16 [4, 640, 2560], P('rep'), parts along dimension 0
- output 3: bfloat16 [4, 2560, 640], P('rep'), parts along dimension 0
- output 4: float32 [4, 640, 2560], P('rep', 'dp'), parts along dimension 0
- output 5: float32 [4, 640, 2560], P('rep', 'dp'), parts along dimension 0
- output 6: float32 [4, 2560, 640], P('rep', 'dp'), parts along dimension 0
- output 7: float32 [4, 640, 2560], P('rep', 'dp'), parts along dimension 0
- output 8: float32 [4, 640, 2560], P('rep', 'dp'), parts along dimension 0
- output 9: float32 [4, 2560, 640], P('rep', 'dp'), parts along dimension 0
There are 2 independent parts. The reference program is written for one: setup_inputs(seed, part) draws one part's arguments, and reference() takes and returns one part's arrays. A program takes and returns all parts, laid end to end along the dimension named above; an argument that names none is the same for every part.
All inputs are finite; a program needn't handle non-finite values.
Results may differ from the reference program's by a relative error of at most 0.022.
Values are sent between devices in bfloat16 or wider.
A program may use at most 2 GiB of HBM per device.

```python
import jax
import jax.numpy as jnp
from jax import lax

SEQUENCES = 16
TOKENS = 2048
D = 640
FF = 2560
LAYERS = 2
NAMES = ("w_gate", "w_up", "w_down")
SHAPES = {"w_gate": (LAYERS, D, FF), "w_up": (LAYERS, D, FF), "w_down": (LAYERS, FF, D)}


def bump(key, n, height):
    away = (jnp.arange(n, dtype=jnp.int32) - jax.random.randint(key, (), 0, n, jnp.int32)) % n
    return jnp.where(away < n // 8, height, 1.0)


def together(key, own, strength):
    shared = jax.random.normal(key, own.shape[1:], jnp.float32)
    return (own + strength * shared) * lax.rsqrt(1 + strength * strength)


def setup_inputs(seed: int = 0, part: int = 0) -> dict:
    kx, kdy, ka, kb, kz, kf, kh, kl, *keys = jax.random.split(jax.random.key(seed), 8 + 3 * len(NAMES))
    kx, kdy, ka, kb = (jax.random.fold_in(k, part) for k in (kx, kdy, ka, kb))
    kw, km, kv = (keys[i::3] for i in range(3))
    shape = (SEQUENCES, TOKENS, D)
    much_x, much_dy = jax.random.uniform(kz, (2,), jnp.float32, 0.0, 1.0)
    loud = 2.0 ** jax.random.uniform(jax.random.fold_in(kz, 1), (), jnp.float32, -1.0, 2.0)
    layers = 2.0 ** jax.random.uniform(kl, (LAYERS, 1, 1), jnp.float32, -1.0, 1.0)
    x = together(ka, jax.random.normal(kx, shape, jnp.float32), much_x) * bump(kf, D, 4.0)
    dy = together(kb, jax.random.normal(kdy, shape, jnp.float32), much_dy)
    drawn = {"x": x.astype(jnp.bfloat16), "dy": (loud * dy * (SEQUENCES * TOKENS) ** -0.5).astype(jnp.bfloat16)}
    for key, name in zip(kw, NAMES, strict=True):
        w = jax.random.normal(key, SHAPES[name], jnp.float32) * SHAPES[name][1] ** -0.5
        drawn[name] = (w * {"w_gate": 1.0, "w_up": bump(kh, FF, 4.0), "w_down": layers}[name]).astype(jnp.bfloat16)
    for key, name in zip(km, NAMES, strict=True):
        drawn[f"m_{name}"] = 0.1 * jax.random.normal(key, SHAPES[name], jnp.float32)
    for key, name in zip(kv, NAMES, strict=True):
        drawn[f"v_{name}"] = jax.random.uniform(key, SHAPES[name], jnp.float32, 0.005, 0.015)
    return drawn


def matmul(a, w):
    return jnp.dot(a, w, preferred_element_type=jnp.float32).astype(jnp.bfloat16)


def normed(h):
    wide = h.astype(jnp.float32)
    scale = lax.rsqrt(jnp.mean(wide**2, -1, keepdims=True) + 1e-6)
    return (wide * scale).astype(jnp.bfloat16)


def layer(h, w):
    a = normed(h)
    gate = jnp.dot(a, w["w_gate"], preferred_element_type=jnp.float32)
    up = jnp.dot(a, w["w_up"], preferred_element_type=jnp.float32)
    return h + matmul((jax.nn.silu(gate) * up).astype(jnp.bfloat16), w["w_down"])


def adamw(w, m, v, g):
    m = 0.9 * m + 0.1 * g
    v = 0.95 * v + 0.05 * g * g
    step = m * lax.rsqrt(v + 1e-8) + 0.1 * w
    return (w - 0.02 * step).astype(jnp.bfloat16), m, v


def clipped(gradients, sum_of_squares, count):
    factor = jnp.minimum(1.0, 0.5 * lax.rsqrt(sum_of_squares / count + 1e-30))
    return [g * factor for g in gradients]


def stack(weights, h):
    return lax.scan(lambda h, w: (layer(h, w), None), h, weights)[0]


def reference(x, dy, w_gate, w_up, w_down, m_w_gate, m_w_up, m_w_down, v_w_gate, v_w_up, v_w_down):
    weights = dict(zip(NAMES, (w_gate, w_up, w_down), strict=True))

    def take(so_far, sequence):
        h, by_y = sequence
        _, back = jax.vjp(lambda w: stack(w, h), weights)
        return jax.tree.map(lambda total, term: total + term.astype(jnp.float32), so_far, back(by_y)[0]), None

    none_yet = {name: jnp.zeros(w.shape, jnp.float32) for name, w in weights.items()}
    by_weights, _ = lax.scan(take, none_yet, (x, dy))
    gradients = [by_weights[name].astype(jnp.bfloat16).astype(jnp.float32) for name in NAMES]
    gradients = clipped(gradients, sum(jnp.sum(g * g) for g in gradients), sum(g.size for g in gradients))
    new = [
        adamw(w.astype(jnp.float32), m, v, g)
        for w, m, v, g in zip((w_gate, w_up, w_down), (m_w_gate, m_w_up, m_w_down), (v_w_gate, v_w_up, v_w_down), gradients, strict=True)
    ]
    return tuple(one[which] for which in range(3) for one in new)
```

```python
import functools

import jax
import jax.numpy as jnp
from jax import lax
from jax.experimental import pallas as pl
from jax.experimental.pallas import tpu as pltpu
from jax.sharding import PartitionSpec as P

F32, BF16 = jnp.float32, jnp.bfloat16
MESH = pl.DeviceIdType.MESH


def matmul(a, w):
    return jnp.dot(a, w, preferred_element_type=F32).astype(BF16)


def normed(h):
    wide = h.astype(F32)
    scale = lax.rsqrt(jnp.mean(wide**2, -1, keepdims=True) + 1e-6)
    return (wide * scale).astype(BF16)


def layer(h, wg, wu, wd):
    a = normed(h)
    gate = jnp.dot(a, wg, preferred_element_type=F32)
    up = jnp.dot(a, wu, preferred_element_type=F32)
    return h + matmul((jax.nn.silu(gate) * up).astype(BF16), wd)


def ring(p):
    return p + (p // 4) * (11 - 2 * p)


def comm_kernel(count, *refs):
    dw, w, m, v = refs[0:6], refs[6:9], refs[9:12], refs[12:15]
    w_out, m_out, v_out = refs[15:18], refs[18:21], refs[21:24]
    (og, od, pg, pd, rg, rd, mg, md, vg, vd, wg, wd, sums,
     load_sem, half_send, half_recv, rs_send, rs_recv, sum_send, sum_recv,
     ag_send, ag_recv, d2d_send, d2d_recv, store_sem) = refs[24:]
    items = [(0, 0), (1, 0), (2, 0), (0, 1), (1, 1), (2, 1)]

    def at(k, big, small):
        which, layer_ = items[k]
        return small.at[layer_] if which == 2 else big.at[2 * layer_ + which]

    rep, dp = lax.axis_index("rep"), lax.axis_index("dp")
    chip, core = dp // 2, dp % 2
    place = ring(chip)
    way = 1 - 2 * core
    to = 2 * ring((place + way + 8) % 8) + core
    partner = dp + way

    barrier = pltpu.get_barrier_semaphore()
    for off in range(1, 16):
        pl.semaphore_signal(barrier, inc=1, device_id=(rep, (dp + off) % 16), device_id_type=MESH)

    loads = []
    for k, (which, layer_) in enumerate(items):
        for n, (src, dst) in enumerate((
            (dw[k].at[:, core], at(k, og, od)),
            (m[which].at[layer_], at(k, mg, md)),
            (v[which].at[layer_], at(k, vg, vd)),
            (w[which].at[layer_, dp], at(k, wg, wd)),
        )):
            c = pltpu.make_async_copy(src, dst, load_sem.at[k, n])
            c.start()
            loads.append(c)
    pl.semaphore_wait(barrier, 15)

    def remote(src, dst, s, r, device):
        return pltpu.make_async_remote_copy(
            src_ref=src, dst_ref=dst, send_sem=s, recv_sem=r, device_id=(rep, device), device_id_type=MESH)

    halves = []
    for k in range(6):
        c = remote(dw[k].at[:, 1 - core], at(k, pg, pd), half_send.at[k], half_recv.at[k], partner)
        c.start()
        halves.append(c)
    for c in loads:
        c.wait()

    def owner(s):
        return ring((place - way * (1 + s) + 16) % 8)

    def ring_copy(k, s, src):
        return remote(src, at(k, rg, rd).at[s], rs_send.at[k, s], rs_recv.at[k, s], to)

    for k in range(6):
        halves[k].wait_recv()
        mine = at(k, og, od).at[owner(0)]
        mine[...] = (mine[...].astype(F32) + at(k, pg, pd).at[owner(0)][...].astype(F32)).astype(BF16)
        ring_copy(k, 0, mine).start()

    def total(k, s):
        who = owner(s + 1)
        return at(k, rg, rd).at[s][...].astype(F32) + (
            at(k, og, od).at[who][...].astype(F32) + at(k, pg, pd).at[who][...].astype(F32))

    def hop(s, _):
        for k in range(6):
            slot = at(k, rg, rd).at[s]
            ring_copy(k, s, slot).wait_recv()
            slot[...] = total(k, s).astype(BF16)
            ring_copy(k, s + 1, slot).start()
        return _

    lax.fori_loop(0, 6, hop, 0)

    squares = jnp.zeros((8, 128), F32)
    for k in range(6):
        slot = at(k, rg, rd).at[6]
        ring_copy(k, 6, slot).wait_recv()
        g = total(k, 6).astype(BF16)
        slot[...] = g
        g = g.astype(F32)
        g = g * g
        part = g[0:8]
        for i in range(1, g.shape[0] // 8):
            part = part + g[8 * i : 8 * i + 8]
        for i in range(part.shape[1] // 128):
            squares = squares + part[:, 128 * i : 128 * i + 128]
    sums.at[dp][...] = squares

    def sum_copy(off):
        return remote(sums.at[dp], sums.at[dp], sum_send.at[off], sum_recv.at[off], (dp + off) % 16)

    for off in range(1, 16):
        sum_copy(off).start()
    for off in range(1, 16):
        sum_copy(off).wait_recv()
    mean = jnp.sum(sums[...]) / count
    factor = jnp.minimum(1.0, 0.5 * lax.rsqrt(jnp.full((8, 128), mean + 1e-30, F32)))[0:1, 0:1]

    def gather_copy(k, s, who):
        which, layer_ = items[k]
        block = w_out[which].at[layer_, who]
        src = at(k, wg, wd) if isinstance(s, int) and s == 0 else block
        return remote(src, block, ag_send.at[k, s], ag_recv.at[k, s], to)

    def d2d_copy(k, s, who):
        which, layer_ = items[k]
        block = w_out[which].at[layer_, who]
        src = at(k, wg, wd) if isinstance(s, int) and s == 0 else block
        return remote(src, block, d2d_send.at[k, s], d2d_recv.at[k, s], partner)

    stores = []
    for k, (which, layer_) in enumerate(items):
        g = at(k, rg, rd).at[6][...].astype(F32) * factor
        mk, vk, wk = at(k, mg, md), at(k, vg, vd), at(k, wg, wd)
        new_m = 0.9 * mk[...] + 0.1 * g
        new_v = 0.95 * vk[...] + 0.05 * g * g
        wide = wk[...].astype(F32)
        wk[...] = (wide - 0.02 * (new_m * lax.rsqrt(new_v + 1e-8) + 0.1 * wide)).astype(BF16)
        mk[...] = new_m
        vk[...] = new_v
        gather_copy(k, 0, dp).start()
        d2d_copy(k, 0, dp).start()
        for n, (src, dst) in enumerate((
            (wk, w_out[which].at[layer_, dp]),
            (mk, m_out[which].at[layer_]),
            (vk, v_out[which].at[layer_]),
        )):
            c = pltpu.make_async_copy(src, dst, store_sem.at[k, n])
            c.start()
            stores.append(c)

    def source(s):
        return 2 * ring((place - way * (1 + s) + 16) % 8) + core

    def gather(s, _):
        for k in range(6):
            who = source(s)
            gather_copy(k, s, who).wait_recv()
            gather_copy(k, s + 1, who).start()
            d2d_copy(k, s + 1, who).start()
        return _

    lax.fori_loop(0, 6, gather, 0)
    for k in range(6):
        who = source(6)
        gather_copy(k, 6, who).wait_recv()
        d2d_copy(k, 7, who).start()

    for c in stores:
        c.wait()
    for k in range(6):
        halves[k].wait_send()
    for off in range(1, 16):
        sum_copy(off).wait_send()

    def drain(s, _):
        for k in range(6):
            ring_copy(k, s, at(k, rg, rd).at[s]).wait_send()
            gather_copy(k, s, dp).wait_send()
            d2d_copy(k, s, dp).wait_send()
            d2d_copy(k, s, dp).wait_recv()
        return _

    lax.fori_loop(0, 7, drain, 0)
    for k in range(6):
        d2d_copy(k, 7, dp).wait_send()
        d2d_copy(k, 7, dp).wait_recv()


def comm(count, grads, weights, m, v):
    G, D = (40, 2560), (160, 640)
    any_ = pl.BlockSpec(memory_space=pl.ANY)
    dma = pltpu.SemaphoreType.DMA

    def two(dtype, lead):
        return [pltpu.VMEM((4, *lead, *G), dtype), pltpu.VMEM((2, *lead, *D), dtype)]

    outs = pl.pallas_call(
        functools.partial(comm_kernel, count),
        out_shape=[
            *(jax.ShapeDtypeStruct(t.shape, BF16) for t in weights),
            *(jax.ShapeDtypeStruct(t.shape, F32) for t in (*m, *v)),
        ],
        in_specs=[any_] * 15,
        out_specs=[any_] * 9,
        scratch_shapes=[
            *two(BF16, (8,)), *two(BF16, (8,)), *two(BF16, (7,)),
            *two(F32, ()), *two(F32, ()), *two(BF16, ()),
            pltpu.VMEM((16, 8, 128), F32),
            dma((6, 4)), dma((6,)), dma((6,)), dma((6, 7)), dma((6, 7)), dma((16,)), dma((16,)),
            dma((6, 7)), dma((6, 7)), dma((6, 8)), dma((6, 8)), dma((6, 3)),
        ],
        compiler_params=pltpu.CompilerParams(
            collective_id=0, has_side_effects=True, vmem_limit_bytes=56 * 1024 * 1024),
    )(*grads, *weights, *m, *v)
    return outs


def solution(mesh):
    def body(x, dy, *arrays):
        weights, m, v = (arrays[i : i + 3] for i in (0, 3, 6))
        x, dy = x[0], dy[0]
        split = [tuple(w[n] for w in weights) for n in range(2)]

        def stack(split):
            h = x
            for one in split:
                h = layer(h, *one)
            return h

        by = jax.vjp(stack, split)[1](dy)[0]
        grads = [g.reshape(8, 2, -1, g.shape[-1]) for one in by for g in one]
        blocks = [w.reshape(2, 16, -1, w.shape[-1]) for w in weights]
        count = float(sum(w.size for w in weights))
        out = comm(count, grads, blocks, m, v)
        return (*(o.reshape(w.shape) for o, w in zip(out[:3], weights)), *out[3:])

    whole, rows = P(None, None, None), P(None, "dp", None)
    return jax.shard_map(
        body,
        mesh=mesh,
        in_specs=(P(("rep", "dp"), None, None),) * 2 + (whole,) * 3 + (rows,) * 6,
        out_specs=(P("rep", None, None),) * 3 + (P("rep", "dp", None),) * 6,
        check_vma=False,
    )
```

```python
import functools

import jax
import jax.numpy as jnp
from jax import lax
from jax.experimental import pallas as pl
from jax.experimental.pallas import tpu as pltpu
from jax.sharding import PartitionSpec as P

F32, BF16 = jnp.float32, jnp.bfloat16
MESH = pl.DeviceIdType.MESH

T, D, FF = 2048, 640, 2560
F = 256
TILES = FF // F
R = 512
STEPS = T // R
HOPS = 7
L0 = TILES + 2
LAST = L0 + TILES


def ring(p):
    return p + (p // 4) * (11 - 2 * p)


def dot(a, b):
    return jnp.dot(a, b, preferred_element_type=F32)


def dot_nt(a, b):
    return lax.dot_general(a, b, (((1,), (1,)), ((), ())), preferred_element_type=F32)


def dot_tn(a, b):
    return lax.dot_general(a, b, (((0,), (0,)), ((), ())), preferred_element_type=F32)


def scale_of(wide):
    return lax.rsqrt(jnp.mean(wide * wide, -1, keepdims=True) + 1e-6)


def where_am_i():
    rep, dp = lax.axis_index("rep"), lax.axis_index("dp")
    chip, core = dp // 2, dp % 2
    way = 1 - 2 * core
    return rep, dp, chip, core, way, ring(chip)


def remote(src, dst, send, recv, rep, device):
    return pltpu.make_async_remote_copy(
        src_ref=src, dst_ref=dst, send_sem=send, recv_sem=recv, device_id=(rep, device), device_id_type=MESH)


def grad_kernel(x_hbm, dy_hbm, wg_hbm, wu_hbm, wd_hbm,
                gg_hbm, gd_hbm, gu_hbm, hid_hbm,
                h, a, a0t, a1t, dy, acc, hid, dg, du, wg, wu, wd, gu,
                own, other, hop, ownd, otherd, hopd, gg, gd,
                io_sem, w_sem, gu_sem, hid_sem,
                half_send, half_recv, hop_send, hop_recv, dhalf_send, dhalf_recv, dhop_send, dhop_recv):
    rep, dp, chip, core, way, place = where_am_i()
    to = 2 * ring((place + way + 8) % 8) + core
    back = 2 * ring((place - way + 8) % 8) + core
    partner = dp + way

    barrier = pltpu.get_barrier_semaphore()
    for device in (to, back, partner):
        pl.semaphore_signal(barrier, inc=1, device_id=(rep, device), device_id_type=MESH)

    x_copy = pltpu.make_async_copy(x_hbm, h, io_sem.at[0])
    dy_copy = pltpu.make_async_copy(dy_hbm, dy, io_sem.at[1])
    x_copy.start()

    def cols(j):
        return pl.ds(pl.multiple_of(j * F, F), F)

    def rows(t):
        return pl.ds(pl.multiple_of(t * R, R), R)

    def w_copies(k):
        layer, j, slot = (k // TILES) % 2, k % TILES, k % 2
        return (
            pltpu.make_async_copy(wg_hbm.at[layer, :, cols(j)], wg.at[slot], w_sem.at[0, slot]),
            pltpu.make_async_copy(wu_hbm.at[layer, :, cols(j)], wu.at[slot], w_sem.at[1, slot]),
            pltpu.make_async_copy(wd_hbm.at[layer, cols(j), :], wd.at[slot], w_sem.at[2, slot]),
        )

    def w_start(k):
        for c in w_copies(k):
            c.start()

    def w_wait(k):
        for c in w_copies(k):
            c.wait()

    def gu_copies(k, out):
        j, t, slot = k // STEPS, k % STEPS, k % 2
        for n in range(2):
            there, here = gu_hbm.at[n, j, rows(t), :], gu.at[slot, n]
            yield pltpu.make_async_copy(here, there, gu_sem.at[n, slot]) if out else pltpu.make_async_copy(
                there, here, gu_sem.at[n, slot])

    def hid_copy(j, out):
        there, here = hid_hbm.at[j], hid.at[j % 2]
        return (pltpu.make_async_copy(here, there, hid_sem.at[j % 2]) if out
                else pltpu.make_async_copy(there, here, hid_sem.at[j % 2]))

    w_start(0)
    x_copy.wait()
    dy_copy.start()

    def owner(s):
        return ring((place - way * (1 + s) + 16) % 8)

    def half(i):
        return remote(own.at[i % TILES, :, 1 - core], other.at[i], half_send.at[i], half_recv.at[i], rep, partner)

    def hop_copy(i, s, src):
        return remote(src, hop.at[i, s], hop_send.at[i, s], hop_recv.at[i, s], rep, to)

    def added(i, who):
        return own.at[i % TILES, who, core][...].astype(F32) + other.at[i, who][...].astype(F32)

    def half_d(d, q):
        rows_ = pl.ds(pl.multiple_of((2 * q + 1 - core) * 160, 32), 160)
        return remote(ownd.at[d, rows_], otherd.at[d, q], dhalf_send.at[d, q], dhalf_recv.at[d, q], rep, partner)

    def hop_copy_d(d, s, src):
        return remote(src, hopd.at[d, s], dhop_send.at[d, s], dhop_recv.at[d, s], rep, to)

    def rows_d(who):
        return pl.ds(pl.multiple_of((2 * who + core) * 160, 32), 160)

    def added_d(d, who):
        return ownd.at[d, rows_d(who)][...].astype(F32) + otherd.at[d, who][...].astype(F32)

    def serve(n):
        for age in range(1, HOPS + 2):
            c = n - age
            late = jnp.where(c >= L0, 1, 0)
            i = c - 2 * late

            @pl.when(((c >= 0) & (c < TILES)) | ((c >= L0) & (c < LAST)))
            def _():
                s = age - 1
                if s == 0:
                    half(i).wait_recv()
                    mine = own.at[i % TILES, owner(0), core]
                    mine[...] = added(i, owner(0)).astype(BF16)
                    hop_copy(i, 0, mine).start()
                else:
                    slot = hop.at[i, s - 1]
                    hop_copy(i, s - 1, slot).wait_recv()
                    who = owner(s)
                    new = (slot[...].astype(F32) + added(i, who)).astype(BF16)
                    if s < HOPS:
                        slot[...] = new
                        hop_copy(i, s, slot).start()
                    else:
                        gg.at[1 - late][:, :, cols(i % TILES)] = new
                        half(i).wait_send()
                        for r in range(HOPS):
                            hop_copy(i, r, slot).wait_send()

    def serve_d(d, age):
        s = age - 1

        @pl.when(s == 0)
        def _():
            for q in range(8):
                half_d(d, q).wait_recv()
            mine = ownd.at[d, rows_d(owner(0))]
            mine[...] = added_d(d, owner(0)).astype(BF16)
            hop_copy_d(d, 0, mine).start()

        @pl.when((s > 0) & (s <= HOPS))
        def _():
            slot = hopd.at[d, s - 1]
            hop_copy_d(d, s - 1, slot).wait_recv()
            new = (slot[...].astype(F32) + added_d(d, owner(s))).astype(BF16)

            @pl.when(s < HOPS)
            def _():
                slot[...] = new
                hop_copy_d(d, s, slot).start()

            @pl.when(s == HOPS)
            def _():
                gd.at[d][...] = new
                for q in range(8):
                    half_d(d, q).wait_send()
                for r in range(HOPS):
                    hop_copy_d(d, r, slot).wait_send()

    def put(i, n, t_, grad):
        g = dot(t_[...], grad[...]).astype(BF16)
        for o in range(16):
            own.at[i % TILES, o // 2, o % 2, n][...] = g[40 * o : 40 * o + 40]

    def norm(t, to_t):
        wide = h[rows(t), :].astype(F32)
        one = (wide * scale_of(wide)).astype(BF16)
        a[rows(t), :] = one
        to_t[:, rows(t)] = one.T
        acc[rows(t), :] = jnp.zeros((R, D), F32)

    def first(t, z):
        norm(t, a0t)
        return z

    lax.fori_loop(0, STEPS, first, 0)

    def forward(j, z):
        slot = j % 2
        w_wait(j)
        w_start(j + 1)

        @pl.when(j >= 2)
        def _():
            hid_copy(j - 2, True).wait()

        def step(t, z):
            k = j * STEPS + t
            gate, up = dot(a[rows(t), :], wg[slot]), dot(a[rows(t), :], wu[slot])

            @pl.when(k >= 2)
            def _():
                for c in gu_copies(k - 2, True):
                    c.wait()

            gu.at[t % 2, 0][...] = gate
            gu.at[t % 2, 1][...] = up
            for c in gu_copies(k, True):
                c.start()
            hidden = (gate * jax.nn.sigmoid(gate) * up).astype(BF16)
            hid.at[slot][rows(t), :] = hidden
            acc[rows(t), :] += dot(hidden, wd[slot])
            return z

        lax.fori_loop(0, STEPS, step, 0)
        hid_copy(j, True).start()
        return z

    lax.fori_loop(0, TILES, forward, 0)
    for k in (TILES * STEPS - 2, TILES * STEPS - 1):
        for c in gu_copies(k, True):
            c.wait()
    for j in (TILES - 2, TILES - 1):
        hid_copy(j, True).wait()

    def second(t, z):
        h[rows(t), :] = (h[rows(t), :].astype(F32) + acc[rows(t), :].astype(BF16).astype(F32)).astype(BF16)
        norm(t, a1t)
        return z

    lax.fori_loop(0, STEPS, second, 0)
    dy_copy.wait()
    pl.semaphore_wait(barrier, 3)

    def back_of(gate, up, by_hidden, slot, t):
        sig = jax.nn.sigmoid(gate)
        silu = gate * sig
        dg[rows(t), :] = (by_hidden * up * (sig + silu * (1.0 - sig))).astype(BF16)
        du[rows(t), :] = (by_hidden * silu).astype(BF16)
        return silu

    def tile(j, z):
        k = TILES + j
        slot = k % 2
        w_wait(k)
        w_start(k + 1)

        def step(t, z):
            gate, up = dot(a[rows(t), :], wg[slot]), dot(a[rows(t), :], wu[slot])
            by_hidden = dot_nt(dy[rows(t), :], wd[slot]).astype(BF16).astype(F32)
            silu = back_of(gate, up, by_hidden, slot, t)
            hid.at[0][rows(t), :] = (silu * up).astype(BF16)
            return z

        lax.fori_loop(0, STEPS, step, 0)
        serve(j)
        put(j, 0, a1t, dg)
        put(j, 1, a1t, du)
        half(j).start()
        ownd.at[1][cols(j), :] = dot_tn(hid[0], dy[...]).astype(BF16)

        def step_a(t, z):
            acc[rows(t), :] += dot_nt(dg[rows(t), :], wg[slot]) + dot_nt(du[rows(t), :], wu[slot])
            return z

        @pl.when(j == 0)
        def _():
            def clear(t, z):
                acc[rows(t), :] = jnp.zeros((R, D), F32)
                return z
            lax.fori_loop(0, STEPS, clear, 0)

        lax.fori_loop(0, STEPS, step_a, 0)
        return z

    lax.fori_loop(0, TILES, tile, 0)
    for q in range(8):
        half_d(1, q).start()
    hid_copy(0, False).start()

    def by_h(t, z):
        by_a = acc[rows(t), :].astype(BF16).astype(F32)
        wide = h[rows(t), :].astype(F32)
        scale = scale_of(wide)
        by_wide = scale * by_a - wide * (scale * scale * scale * jnp.mean(by_a * wide, -1, keepdims=True))
        dy[rows(t), :] = (dy[rows(t), :].astype(F32) + by_wide.astype(BF16).astype(F32)).astype(BF16)
        return z

    lax.fori_loop(0, STEPS, by_h, 0)

    def down(r, z):
        def one(jj, z):
            j = r * (TILES // 2) + jj
            hid_copy(j, False).wait()

            @pl.when(j + 1 < TILES)
            def _():
                hid_copy(j + 1, False).start()

            ownd.at[0][cols(j), :] = dot_tn(hid[j % 2], dy[...]).astype(BF16)
            return z

        lax.fori_loop(0, TILES // 2, one, 0)
        serve(TILES + r)
        serve_d(1, 1 + r)
        return z

    for c in gu_copies(0, False):
        c.start()
    lax.fori_loop(0, 2, down, 0)
    for q in range(8):
        half_d(0, q).start()

    def tile0(j, z):
        k = 2 * TILES + j
        slot = k % 2
        w_wait(k)

        @pl.when(j + 1 < TILES)
        def _():
            w_start(k + 1)

        def step(t, z):
            n = j * STEPS + t
            by_hidden = dot_nt(dy[rows(t), :], wd[slot]).astype(BF16).astype(F32)
            for c in gu_copies(n, False):
                c.wait()

            @pl.when(n + 1 < TILES * STEPS)
            def _():
                for c in gu_copies(n + 1, False):
                    c.start()

            back_of(gu[t % 2, 0], gu[t % 2, 1], by_hidden, slot, t)
            return z

        lax.fori_loop(0, STEPS, step, 0)
        serve(L0 + j)
        serve_d(1, 3 + j)
        serve_d(0, 1 + j)
        put(TILES + j, 0, a0t, dg)
        put(TILES + j, 1, a0t, du)
        half(TILES + j).start()
        return z

    lax.fori_loop(0, TILES, tile0, 0)

    def drain(r, z):
        serve(LAST + r)
        return z

    lax.fori_loop(0, HOPS + 1, drain, 0)
    out = [pltpu.make_async_copy(gg, gg_hbm, io_sem.at[0]), pltpu.make_async_copy(gd, gd_hbm, io_sem.at[1])]
    for c in out:
        c.start()
    for c in out:
        c.wait()


def grads(x, dy, wg, wu, wd):
    any_ = pl.BlockSpec(memory_space=pl.ANY)
    dma, vmem = pltpu.SemaphoreType.DMA, pltpu.VMEM
    s = jax.ShapeDtypeStruct
    block = (2, 40, F)
    out = pl.pallas_call(
        grad_kernel,
        out_shape=[s((2, 2, 40, FF), BF16), s((2, 160, D), BF16),
                   s((2, TILES, T, F), F32), s((TILES, T, F), BF16)],
        in_specs=[any_] * 5,
        out_specs=[any_] * 4,
        scratch_shapes=[
            vmem((T, D), BF16), vmem((T, D), BF16), vmem((D, T), BF16), vmem((D, T), BF16), vmem((T, D), BF16),
            vmem((T, D), F32), vmem((2, T, F), BF16), vmem((T, F), BF16), vmem((T, F), BF16),
            vmem((2, D, F), BF16), vmem((2, D, F), BF16), vmem((2, F, D), BF16), vmem((2, 2, R, F), F32),
            vmem((TILES, 8, 2, *block), BF16), vmem((2 * TILES, 8, *block), BF16), vmem((2 * TILES, HOPS, *block), BF16),
            vmem((2, FF, D), BF16), vmem((2, 8, 160, D), BF16), vmem((2, HOPS, 160, D), BF16),
            vmem((2, 2, 40, FF), BF16), vmem((2, 160, D), BF16),
            dma((2,)), dma((3, 2)), dma((2, 2)), dma((2,)),
            dma((2 * TILES,)), dma((2 * TILES,)), dma((2 * TILES, HOPS)), dma((2 * TILES, HOPS)),
            dma((2, 8)), dma((2, 8)), dma((2, HOPS)), dma((2, HOPS)),
        ],
        compiler_params=pltpu.CompilerParams(
            collective_id=1, has_side_effects=True, vmem_limit_bytes=67043328),
    )(x, dy, wg, wu, wd)
    return out[:2]


def update_kernel(count, *refs):
    gg_hbm, gd_hbm, w, m, v = refs[0], refs[1], refs[2:5], refs[5:8], refs[8:11]
    w_out, m_out, v_out = refs[11:14], refs[14:17], refs[17:20]
    (gg, gd, mg, md, vg, vd, wg, wd, sums, g_sem, load_sem, sum_send, sum_recv,
     ag_send, ag_recv, d2d_send, d2d_recv, store_sem) = refs[20:]
    items = [(0, 0), (1, 0), (2, 0), (0, 1), (1, 1), (2, 1)]

    def at(k, big, small):
        which, layer_ = items[k]
        return small.at[layer_] if which == 2 else big.at[layer_, which]

    rep, dp, chip, core, way, place = where_am_i()
    to = 2 * ring((place + way + 8) % 8) + core
    partner = dp + way

    barrier = pltpu.get_barrier_semaphore()
    for off in range(1, 16):
        pl.semaphore_signal(barrier, inc=1, device_id=(rep, (dp + off) % 16), device_id_type=MESH)

    g_loads = [pltpu.make_async_copy(gg_hbm, gg, g_sem.at[0]), pltpu.make_async_copy(gd_hbm, gd, g_sem.at[1])]
    for c in g_loads:
        c.start()
    loads = []
    for k, (which, layer_) in enumerate(items):
        for n, (src, dst) in enumerate((
            (m[which].at[layer_], at(k, mg, md)),
            (v[which].at[layer_], at(k, vg, vd)),
            (w[which].at[layer_, dp], at(k, wg, wd)),
        )):
            c = pltpu.make_async_copy(src, dst, load_sem.at[k, n])
            c.start()
            loads.append(c)
    for c in g_loads:
        c.wait()

    squares = jnp.zeros((8, 128), F32)
    for k in range(6):
        g = at(k, gg, gd)[...].astype(F32)
        g = g * g
        part = g[0:8]
        for i in range(1, g.shape[0] // 8):
            part = part + g[8 * i : 8 * i + 8]
        for i in range(part.shape[1] // 128):
            squares = squares + part[:, 128 * i : 128 * i + 128]
    sums.at[dp][...] = squares
    pl.semaphore_wait(barrier, 15)

    def sum_copy(off):
        return remote(sums.at[dp], sums.at[dp], sum_send.at[off], sum_recv.at[off], rep, (dp + off) % 16)

    for off in range(1, 16):
        sum_copy(off).start()
    for c in loads:
        c.wait()
    for off in range(1, 16):
        sum_copy(off).wait_recv()
    mean = jnp.sum(sums[...]) / count
    factor = jnp.minimum(1.0, 0.5 * lax.rsqrt(jnp.full((8, 128), mean + 1e-30, F32)))[0:1, 0:1]

    def block(k, who):
        which, layer_ = items[k]
        return w_out[which].at[layer_, who]

    def gather_copy(k, s, who, src=None):
        src = block(k, who) if src is None else src
        return remote(src, block(k, who), ag_send.at[k, s], ag_recv.at[k, s], rep, to)

    def d2d_copy(k, s, who, src=None):
        src = block(k, who) if src is None else src
        return remote(src, block(k, who), d2d_send.at[k, s], d2d_recv.at[k, s], rep, partner)

    stores = []
    for k, (which, layer_) in enumerate(items):
        g = at(k, gg, gd)[...].astype(F32) * factor
        mk, vk, wk = at(k, mg, md), at(k, vg, vd), at(k, wg, wd)
        new_m = 0.9 * mk[...] + 0.1 * g
        new_v = 0.95 * vk[...] + 0.05 * g * g
        wide = wk[...].astype(F32)
        wk[...] = (wide - 0.02 * (new_m * lax.rsqrt(new_v + 1e-8) + 0.1 * wide)).astype(BF16)
        mk[...] = new_m
        vk[...] = new_v
        gather_copy(k, 0, dp, wk).start()
        d2d_copy(k, 0, dp, wk).start()
        for n, (src, dst) in enumerate((
            (wk, block(k, dp)), (mk, m_out[which].at[layer_]), (vk, v_out[which].at[layer_]))):
            c = pltpu.make_async_copy(src, dst, store_sem.at[k, n])
            c.start()
            stores.append(c)

    def source(s):
        return 2 * ring((place - way * (1 + s) + 16) % 8) + core

    def gather(s, z):
        for k in range(6):
            who = source(s)
            gather_copy(k, s, who).wait_recv()
            gather_copy(k, s + 1, who).start()
            d2d_copy(k, s + 1, who).start()
        return z

    lax.fori_loop(0, 6, gather, 0)
    for k in range(6):
        who = source(6)
        gather_copy(k, 6, who).wait_recv()
        d2d_copy(k, 7, who).start()

    for c in stores:
        c.wait()
    for off in range(1, 16):
        sum_copy(off).wait_send()

    def drain(s, z):
        for k in range(6):
            gather_copy(k, s, dp).wait_send()
            d2d_copy(k, s, dp).wait_send()
            d2d_copy(k, s, dp).wait_recv()
        return z

    lax.fori_loop(0, 7, drain, 0)
    for k in range(6):
        d2d_copy(k, 7, dp).wait_send()
        d2d_copy(k, 7, dp).wait_recv()


def update(count, gg, gd, weights, m, v):
    G, S = (2, 2, 40, FF), (2, 160, D)
    any_ = pl.BlockSpec(memory_space=pl.ANY)
    dma, vmem = pltpu.SemaphoreType.DMA, pltpu.VMEM
    return pl.pallas_call(
        functools.partial(update_kernel, count),
        out_shape=[
            *(jax.ShapeDtypeStruct(t.shape, BF16) for t in weights),
            *(jax.ShapeDtypeStruct(t.shape, F32) for t in (*m, *v)),
        ],
        in_specs=[any_] * 11,
        out_specs=[any_] * 9,
        scratch_shapes=[
            vmem(G, BF16), vmem(S, BF16), vmem(G, F32), vmem(S, F32), vmem(G, F32), vmem(S, F32), vmem(G, BF16), vmem(S, BF16),
            vmem((16, 8, 128), F32),
            dma((2,)), dma((6, 3)), dma((16,)), dma((16,)),
            dma((6, 7)), dma((6, 7)), dma((6, 8)), dma((6, 8)), dma((6, 3)),
        ],
        compiler_params=pltpu.CompilerParams(
            collective_id=0, has_side_effects=True, vmem_limit_bytes=24 * 1024 * 1024),
    )(gg, gd, *weights, *m, *v)


def solution(mesh):
    def body(x, dy, *arrays):
        weights, m, v = (arrays[i : i + 3] for i in (0, 3, 6))
        gg, gd = grads(x[0], dy[0], *weights)
        blocks = [w.reshape(2, 16, -1, w.shape[-1]) for w in weights]
        count = float(sum(w.size for w in weights))
        out = update(count, gg, gd, blocks, m, v)
        return (*(o.reshape(w.shape) for o, w in zip(out[:3], weights)), *out[3:])

    whole, rows = P(None, None, None), P(None, "dp", None)
    return jax.shard_map(
        body,
        mesh=mesh,
        in_specs=(P(("rep", "dp"), None, None),) * 2 + (whole,) * 3 + (rows,) * 6,
        out_specs=(P("rep", None, None),) * 3 + (P("rep", "dp", None),) * 6,
        check_vma=False,
    )
```

```python
import functools

import jax
import jax.numpy as jnp
from jax import lax
from jax.experimental import pallas as pl
from jax.experimental.pallas import tpu as pltpu
from jax.sharding import PartitionSpec as P

F32, BF16 = jnp.float32, jnp.bfloat16
MESH = pl.DeviceIdType.MESH

T, D, FF = 2048, 640, 2560
F = 256
TILES = FF // F
R = 512
STEPS = T // R
DEPTH = 4
HOPS = 7
L0 = TILES + 2
LAST = L0 + TILES


def ring(p):
    return p + (p // 4) * (11 - 2 * p)


def dot(a, b):
    return jnp.dot(a, b, preferred_element_type=F32)


def dot_nt(a, b):
    return lax.dot_general(a, b, (((1,), (1,)), ((), ())), preferred_element_type=F32)


def dot_tn(a, b):
    return lax.dot_general(a, b, (((0,), (0,)), ((), ())), preferred_element_type=F32)


def sigmoid(x):
    return jax.nn.sigmoid(x)


def scale_of(wide):
    return lax.rsqrt(jnp.mean(wide * wide, -1, keepdims=True) + 1e-6)


def where_am_i():
    rep, dp = lax.axis_index("rep"), lax.axis_index("dp")
    chip, core = dp // 2, dp % 2
    way = 1 - 2 * core
    return rep, dp, chip, core, way, ring(chip)


def remote(src, dst, send, recv, rep, device):
    return pltpu.make_async_remote_copy(
        src_ref=src, dst_ref=dst, send_sem=send, recv_sem=recv, device_id=(rep, device), device_id_type=MESH)


def grad_kernel(x_hbm, dy_hbm, wg_hbm, wu_hbm, wd_hbm,
                gg_hbm, gd_hbm, gu_hbm, hid_hbm,
                h, a, a0t, a1t, dy, acc, hid, dg, du, wg, wu, wd, gu,
                own, other, hop, ownd, otherd, hopd, gg, gd,
                io_sem, w_sem, gu_sem, hid_sem,
                half_send, half_recv, hop_send, hop_recv, dhalf_send, dhalf_recv, dhop_send, dhop_recv):
    rep, dp, chip, core, way, place = where_am_i()
    to = 2 * ring((place + way + 8) % 8) + core
    back = 2 * ring((place - way + 8) % 8) + core
    partner = dp + way

    barrier = pltpu.get_barrier_semaphore()
    for device in (to, back, partner):
        pl.semaphore_signal(barrier, inc=1, device_id=(rep, device), device_id_type=MESH)

    x_copy = pltpu.make_async_copy(x_hbm, h, io_sem.at[0])
    dy_copy = pltpu.make_async_copy(dy_hbm, dy, io_sem.at[1])
    x_copy.start()

    def cols(j):
        return pl.ds(pl.multiple_of(j * F, F), F)

    def rows(t):
        return pl.ds(t * R, R) if isinstance(t, int) else pl.ds(pl.multiple_of(t * R, R), R)

    def w_copies(k):
        layer, j, slot = (k // TILES) % 2, k % TILES, k % 2
        return (
            pltpu.make_async_copy(wg_hbm.at[layer, :, cols(j)], wg.at[slot], w_sem.at[0, slot]),
            pltpu.make_async_copy(wu_hbm.at[layer, :, cols(j)], wu.at[slot], w_sem.at[1, slot]),
            pltpu.make_async_copy(wd_hbm.at[layer, cols(j), :], wd.at[slot], w_sem.at[2, slot]),
        )

    def w_start(k):
        for c in w_copies(k):
            c.start()

    def w_wait(k):
        for c in w_copies(k):
            c.wait()

    def gu_copies(k, out):
        j, t, slot = k // STEPS, k % STEPS, k % DEPTH
        for n in range(2):
            there, here = gu_hbm.at[n, j, rows(t), :], gu.at[slot, n]
            yield pltpu.make_async_copy(here, there, gu_sem.at[n, slot]) if out else pltpu.make_async_copy(
                there, here, gu_sem.at[n, slot])

    def hid_copy(j, out):
        there, here = hid_hbm.at[j], hid.at[j % 3]
        return (pltpu.make_async_copy(here, there, hid_sem.at[j % 3]) if out
                else pltpu.make_async_copy(there, here, hid_sem.at[j % 3]))

    w_start(0)
    x_copy.wait()
    dy_copy.start()

    def owner(s):
        return ring((place - way * (1 + s) + 16) % 8)

    def half(i):
        return remote(own.at[i % TILES, :, 1 - core], other.at[i], half_send.at[i], half_recv.at[i], rep, partner)

    def hop_copy(i, s, src):
        return remote(src, hop.at[i, s], hop_send.at[i, s], hop_recv.at[i, s], rep, to)

    def added(i, who):
        return own.at[i % TILES, who, core][...].astype(F32) + other.at[i, who][...].astype(F32)

    def half_d(d, q):
        rows_ = pl.ds(pl.multiple_of((2 * q + 1 - core) * 160, 32), 160)
        return remote(ownd.at[d, rows_], otherd.at[d, q], dhalf_send.at[d, q], dhalf_recv.at[d, q], rep, partner)

    def hop_copy_d(d, s, src):
        return remote(src, hopd.at[d, s], dhop_send.at[d, s], dhop_recv.at[d, s], rep, to)

    def rows_d(who):
        return pl.ds(pl.multiple_of((2 * who + core) * 160, 32), 160)

    def added_d(d, who):
        return ownd.at[d, rows_d(who)][...].astype(F32) + otherd.at[d, who][...].astype(F32)

    def serve(n):
        for age in range(1, HOPS + 2):
            c = n - age
            late = jnp.where(c >= L0, 1, 0)
            i = c - 2 * late

            @pl.when(((c >= 0) & (c < TILES)) | ((c >= L0) & (c < LAST)))
            def _():
                s = age - 1
                if s == 0:
                    half(i).wait_recv()
                    mine = own.at[i % TILES, owner(0), core]
                    mine[...] = added(i, owner(0)).astype(BF16)
                    hop_copy(i, 0, mine).start()
                else:
                    slot = hop.at[i, s - 1]
                    hop_copy(i, s - 1, slot).wait_recv()
                    who = owner(s)
                    new = (slot[...].astype(F32) + added(i, who)).astype(BF16)
                    if s < HOPS:
                        slot[...] = new
                        hop_copy(i, s, slot).start()
                    else:
                        gg.at[1 - late][:, :, cols(i % TILES)] = new
                        half(i).wait_send()
                        for r in range(HOPS):
                            hop_copy(i, r, slot).wait_send()

    def serve_d(d, age):
        s = age - 1

        @pl.when(s == 0)
        def _():
            for q in range(8):
                half_d(d, q).wait_recv()
            mine = ownd.at[d, rows_d(owner(0))]
            mine[...] = added_d(d, owner(0)).astype(BF16)
            hop_copy_d(d, 0, mine).start()

        @pl.when((s > 0) & (s <= HOPS))
        def _():
            slot = hopd.at[d, s - 1]
            hop_copy_d(d, s - 1, slot).wait_recv()
            new = (slot[...].astype(F32) + added_d(d, owner(s))).astype(BF16)

            @pl.when(s < HOPS)
            def _():
                slot[...] = new
                hop_copy_d(d, s, slot).start()

            @pl.when(s == HOPS)
            def _():
                gd.at[d][...] = new
                for q in range(8):
                    half_d(d, q).wait_send()
                for r in range(HOPS):
                    hop_copy_d(d, r, slot).wait_send()

    def put(i, n, t_, grad):
        g = dot(t_[...], grad[...]).astype(BF16)
        for o in range(16):
            own.at[i % TILES, o // 2, o % 2, n][...] = g[40 * o : 40 * o + 40]

    def norm(t, to_t):
        wide = h[rows(t), :].astype(F32)
        one = (wide * scale_of(wide)).astype(BF16)
        a[rows(t), :] = one
        to_t[:, rows(t)] = one.T
        acc[rows(t), :] = jnp.zeros((R, D), F32)

    def first(t, z):
        norm(t, a0t)
        return z

    lax.fori_loop(0, STEPS, first, 0)

    hid.at[2][rows(STEPS - 1), :] = jnp.zeros((R, F), BF16)
    wd.at[1][...] = jnp.zeros((F, D), BF16)

    def forward(j, z):
        w_wait(j)

        @pl.when(j >= 3)
        def _():
            hid_copy(j - 3, True).wait()

        def step(t, before):
            k = j * STEPS + t
            h_slot, w_slot, t_before = before
            acc[rows(t_before), :] += dot(hid[h_slot, rows(t_before), :], wd[w_slot])
            gate, up = dot(a[rows(t), :], wg[j % 2]), dot(a[rows(t), :], wu[j % 2])
            hidden = (gate * sigmoid(gate) * up).astype(BF16)

            @pl.when(k >= DEPTH)
            def _():
                for c in gu_copies(k - DEPTH, True):
                    c.wait()

            gu.at[k % DEPTH, 0][...] = gate
            gu.at[k % DEPTH, 1][...] = up
            hid.at[j % 3][rows(t), :] = hidden
            for c in gu_copies(k, True):
                c.start()

        step(0, ((j + 2) % 3, (j + 1) % 2, STEPS - 1))
        w_start(j + 1)
        for t in range(1, STEPS):
            step(t, (j % 3, j % 2, t - 1))
        hid_copy(j, True).start()
        return z

    lax.fori_loop(0, TILES, forward, 0)
    acc[rows(STEPS - 1), :] += dot(hid[(TILES - 1) % 3, rows(STEPS - 1), :], wd[(TILES - 1) % 2])
    for k in range(TILES * STEPS - DEPTH, TILES * STEPS):
        for c in gu_copies(k, True):
            c.wait()
    for j in range(TILES - 3, TILES):
        hid_copy(j, True).wait()

    def second(t, z):
        h[rows(t), :] = (h[rows(t), :].astype(F32) + acc[rows(t), :].astype(BF16).astype(F32)).astype(BF16)
        norm(t, a1t)
        return z

    lax.fori_loop(0, STEPS, second, 0)
    dy_copy.wait()
    pl.semaphore_wait(barrier, 3)

    def back_of(gate, up, by_hidden, slot, t):
        sig = sigmoid(gate)
        silu = gate * sig
        dg[rows(t), :] = (by_hidden * up * (sig + silu * (1.0 - sig))).astype(BF16)
        du[rows(t), :] = (by_hidden * silu).astype(BF16)
        return silu

    def tile(j, z):
        k = TILES + j
        slot = k % 2
        w_wait(k)
        w_start(k + 1)

        def step(t, z):
            gate, up = dot(a[rows(t), :], wg[slot]), dot(a[rows(t), :], wu[slot])
            by_hidden = dot_nt(dy[rows(t), :], wd[slot]).astype(BF16).astype(F32)
            silu = back_of(gate, up, by_hidden, slot, t)
            hid.at[0][rows(t), :] = (silu * up).astype(BF16)
            return z

        for t in range(STEPS):
            step(t, 0)
        serve(j)
        put(j, 0, a1t, dg)
        put(j, 1, a1t, du)
        half(j).start()
        ownd.at[1][cols(j), :] = dot_tn(hid[0], dy[...]).astype(BF16)

        def step_a(t, z):
            acc[rows(t), :] += dot_nt(dg[rows(t), :], wg[slot]) + dot_nt(du[rows(t), :], wu[slot])
            return z

        @pl.when(j == 0)
        def _():
            def clear(t, z):
                acc[rows(t), :] = jnp.zeros((R, D), F32)
                return z
            lax.fori_loop(0, STEPS, clear, 0)

        lax.fori_loop(0, STEPS, step_a, 0)
        return z

    lax.fori_loop(0, TILES, tile, 0)
    for q in range(8):
        half_d(1, q).start()
    hid_copy(0, False).start()
    hid_copy(1, False).start()
    for k in range(DEPTH - 1):
        for c in gu_copies(k, False):
            c.start()

    def by_h(t, z):
        by_a = acc[rows(t), :].astype(BF16).astype(F32)
        wide = h[rows(t), :].astype(F32)
        scale = scale_of(wide)
        by_wide = scale * by_a - wide * (scale * scale * scale * jnp.mean(by_a * wide, -1, keepdims=True))
        dy[rows(t), :] = (dy[rows(t), :].astype(F32) + by_wide.astype(BF16).astype(F32)).astype(BF16)
        return z

    lax.fori_loop(0, STEPS, by_h, 0)

    def down(r, z):
        def one(jj, z):
            j = r * (TILES // 2) + jj
            hid_copy(j, False).wait()

            @pl.when(j + 2 < TILES)
            def _():
                hid_copy(j + 2, False).start()

            ownd.at[0][cols(j), :] = dot_tn(hid[j % 3], dy[...]).astype(BF16)
            return z

        lax.fori_loop(0, TILES // 2, one, 0)
        serve(TILES + r)
        serve_d(1, 1 + r)
        return z

    lax.fori_loop(0, 2, down, 0)
    for q in range(8):
        half_d(0, q).start()

    def tile0(j, z):
        k = 2 * TILES + j
        slot = k % 2
        w_wait(k)

        @pl.when(j + 1 < TILES)
        def _():
            w_start(k + 1)

        def step(t, z):
            n = j * STEPS + t
            by_hidden = dot_nt(dy[rows(t), :], wd[slot]).astype(BF16).astype(F32)
            for c in gu_copies(n, False):
                c.wait()

            @pl.when(n + DEPTH - 1 < TILES * STEPS)
            def _():
                for c in gu_copies(n + DEPTH - 1, False):
                    c.start()

            back_of(gu[n % DEPTH, 0], gu[n % DEPTH, 1], by_hidden, slot, t)
            return z

        lax.fori_loop(0, STEPS, step, 0)
        serve(L0 + j)
        serve_d(1, 3 + j)
        serve_d(0, 1 + j)
        put(TILES + j, 0, a0t, dg)
        put(TILES + j, 1, a0t, du)
        half(TILES + j).start()
        return z

    lax.fori_loop(0, TILES, tile0, 0)

    def drain(r, z):
        serve(LAST + r)
        return z

    lax.fori_loop(0, HOPS + 1, drain, 0)
    out = [pltpu.make_async_copy(gg, gg_hbm, io_sem.at[0]), pltpu.make_async_copy(gd, gd_hbm, io_sem.at[1])]
    for c in out:
        c.start()
    for c in out:
        c.wait()


def grads(x, dy, wg, wu, wd):
    any_ = pl.BlockSpec(memory_space=pl.ANY)
    dma, vmem = pltpu.SemaphoreType.DMA, pltpu.VMEM
    s = jax.ShapeDtypeStruct
    block = (2, 40, F)
    out = pl.pallas_call(
        grad_kernel,
        out_shape=[s((2, 2, 40, FF), BF16), s((2, 160, D), BF16),
                   s((2, TILES, T, F), F32), s((TILES, T, F), BF16)],
        in_specs=[any_] * 5,
        out_specs=[any_] * 4,
        scratch_shapes=[
            vmem((T, D), BF16), vmem((T, D), BF16), vmem((D, T), BF16), vmem((D, T), BF16), vmem((T, D), BF16),
            vmem((T, D), F32), vmem((3, T, F), BF16), vmem((T, F), BF16), vmem((T, F), BF16),
            vmem((2, D, F), BF16), vmem((2, D, F), BF16), vmem((2, F, D), BF16), vmem((DEPTH, 2, R, F), F32),
            vmem((TILES, 8, 2, *block), BF16), vmem((2 * TILES, 8, *block), BF16), vmem((2 * TILES, HOPS, *block), BF16),
            vmem((2, FF, D), BF16), vmem((2, 8, 160, D), BF16), vmem((2, HOPS, 160, D), BF16),
            vmem((2, 2, 40, FF), BF16), vmem((2, 160, D), BF16),
            dma((2,)), dma((3, 2)), dma((2, DEPTH)), dma((3,)),
            dma((2 * TILES,)), dma((2 * TILES,)), dma((2 * TILES, HOPS)), dma((2 * TILES, HOPS)),
            dma((2, 8)), dma((2, 8)), dma((2, HOPS)), dma((2, HOPS)),
        ],
        compiler_params=pltpu.CompilerParams(
            collective_id=1, has_side_effects=True, vmem_limit_bytes=67043328),
    )(x, dy, wg, wu, wd)
    return out[:2]


def update_kernel(count, *refs):
    gg_hbm, gd_hbm, w, m, v = refs[0], refs[1], refs[2:5], refs[5:8], refs[8:11]
    w_out, m_out, v_out = refs[11:14], refs[14:17], refs[17:20]
    (gg, gd, mg, md, vg, vd, wg, wd, sums, g_sem, load_sem, sum_send, sum_recv,
     ag_send, ag_recv, d2d_send, d2d_recv, store_sem) = refs[20:]
    items = [(0, 0), (1, 0), (2, 0), (0, 1), (1, 1), (2, 1)]

    def at(k, big, small):
        which, layer_ = items[k]
        return small.at[layer_] if which == 2 else big.at[layer_, which]

    rep, dp, chip, core, way, place = where_am_i()
    to = 2 * ring((place + way + 8) % 8) + core
    partner = dp + way

    barrier = pltpu.get_barrier_semaphore()
    for off in range(1, 16):
        pl.semaphore_signal(barrier, inc=1, device_id=(rep, (dp + off) % 16), device_id_type=MESH)

    g_loads = [pltpu.make_async_copy(gg_hbm, gg, g_sem.at[0]), pltpu.make_async_copy(gd_hbm, gd, g_sem.at[1])]
    for c in g_loads:
        c.start()
    loads = []
    for k, (which, layer_) in enumerate(items):
        for n, (src, dst) in enumerate((
            (m[which].at[layer_], at(k, mg, md)),
            (v[which].at[layer_], at(k, vg, vd)),
            (w[which].at[layer_, dp], at(k, wg, wd)),
        )):
            c = pltpu.make_async_copy(src, dst, load_sem.at[k, n])
            c.start()
            loads.append(c)
    for c in g_loads:
        c.wait()

    squares = jnp.zeros((8, 128), F32)
    for k in range(6):
        g = at(k, gg, gd)[...].astype(F32)
        g = g * g
        part = g[0:8]
        for i in range(1, g.shape[0] // 8):
            part = part + g[8 * i : 8 * i + 8]
        for i in range(part.shape[1] // 128):
            squares = squares + part[:, 128 * i : 128 * i + 128]
    sums.at[dp][...] = squares
    pl.semaphore_wait(barrier, 15)

    def sum_copy(off):
        return remote(sums.at[dp], sums.at[dp], sum_send.at[off], sum_recv.at[off], rep, (dp + off) % 16)

    for off in range(1, 16):
        sum_copy(off).start()
    for c in loads:
        c.wait()
    for off in range(1, 16):
        sum_copy(off).wait_recv()
    mean = jnp.sum(sums[...]) / count
    factor = jnp.minimum(1.0, 0.5 * lax.rsqrt(jnp.full((8, 128), mean + 1e-30, F32)))[0:1, 0:1]

    def block(k, who):
        which, layer_ = items[k]
        return w_out[which].at[layer_, who]

    def gather_copy(k, s, who, src=None):
        src = block(k, who) if src is None else src
        return remote(src, block(k, who), ag_send.at[k, s], ag_recv.at[k, s], rep, to)

    def d2d_copy(k, s, who, src=None):
        src = block(k, who) if src is None else src
        return remote(src, block(k, who), d2d_send.at[k, s], d2d_recv.at[k, s], rep, partner)

    stores = []
    for k, (which, layer_) in enumerate(items):
        g = at(k, gg, gd)[...].astype(F32) * factor
        mk, vk, wk = at(k, mg, md), at(k, vg, vd), at(k, wg, wd)
        new_m = 0.9 * mk[...] + 0.1 * g
        new_v = 0.95 * vk[...] + 0.05 * g * g
        wide = wk[...].astype(F32)
        wk[...] = (wide - 0.02 * (new_m * lax.rsqrt(new_v + 1e-8) + 0.1 * wide)).astype(BF16)
        mk[...] = new_m
        vk[...] = new_v
        gather_copy(k, 0, dp, wk).start()
        d2d_copy(k, 0, dp, wk).start()
        for n, (src, dst) in enumerate((
            (wk, block(k, dp)), (mk, m_out[which].at[layer_]), (vk, v_out[which].at[layer_]))):
            c = pltpu.make_async_copy(src, dst, store_sem.at[k, n])
            c.start()
            stores.append(c)

    def source(s):
        return 2 * ring((place - way * (1 + s) + 16) % 8) + core

    def gather(s, z):
        for k in range(6):
            who = source(s)
            gather_copy(k, s, who).wait_recv()
            gather_copy(k, s + 1, who).start()
            d2d_copy(k, s + 1, who).start()
        return z

    lax.fori_loop(0, 6, gather, 0)
    for k in range(6):
        who = source(6)
        gather_copy(k, 6, who).wait_recv()
        d2d_copy(k, 7, who).start()

    for c in stores:
        c.wait()
    for off in range(1, 16):
        sum_copy(off).wait_send()

    def drain(s, z):
        for k in range(6):
            gather_copy(k, s, dp).wait_send()
            d2d_copy(k, s, dp).wait_send()
            d2d_copy(k, s, dp).wait_recv()
        return z

    lax.fori_loop(0, 7, drain, 0)
    for k in range(6):
        d2d_copy(k, 7, dp).wait_send()
        d2d_copy(k, 7, dp).wait_recv()


def update(count, gg, gd, weights, m, v):
    G, S = (2, 2, 40, FF), (2, 160, D)
    any_ = pl.BlockSpec(memory_space=pl.ANY)
    dma, vmem = pltpu.SemaphoreType.DMA, pltpu.VMEM
    return pl.pallas_call(
        functools.partial(update_kernel, count),
        out_shape=[
            *(jax.ShapeDtypeStruct(t.shape, BF16) for t in weights),
            *(jax.ShapeDtypeStruct(t.shape, F32) for t in (*m, *v)),
        ],
        in_specs=[pl.BlockSpec(memory_space=pltpu.HBM)] * 11,
        out_specs=[any_] * 9,
        scratch_shapes=[
            vmem(G, BF16), vmem(S, BF16), vmem(G, F32), vmem(S, F32), vmem(G, F32), vmem(S, F32), vmem(G, BF16), vmem(S, BF16),
            vmem((16, 8, 128), F32),
            dma((2,)), dma((6, 3)), dma((16,)), dma((16,)),
            dma((6, 7)), dma((6, 7)), dma((6, 8)), dma((6, 8)), dma((6, 3)),
        ],
        compiler_params=pltpu.CompilerParams(
            collective_id=0, has_side_effects=True, vmem_limit_bytes=16 * 1024 * 1024),
    )(*(pltpu.with_memory_space_constraint(t, pltpu.HBM) for t in (gg, gd, *weights, *m, *v)))


def out_kernel(n, *refs):
    copies = [pltpu.make_async_copy(refs[i], refs[n + i], refs[2 * n].at[i]) for i in range(n)]
    for c in copies:
        c.start()
    for c in copies:
        c.wait()


def put_out(arrays):
    n = len(arrays)
    return pl.pallas_call(
        functools.partial(out_kernel, n),
        out_shape=[jax.ShapeDtypeStruct(t.shape, t.dtype) for t in arrays],
        in_specs=[pl.BlockSpec(memory_space=pl.ANY)] * n,
        out_specs=[pl.BlockSpec(memory_space=pltpu.HBM)] * n,
        scratch_shapes=[pltpu.SemaphoreType.DMA((n,))],
        compiler_params=pltpu.CompilerParams(vmem_limit_bytes=1024 * 1024),
    )(*arrays)


def solution(mesh):
    def body(x, dy, *arrays):
        weights, m, v = (arrays[i : i + 3] for i in (0, 3, 6))
        gg, gd = grads(x[0], dy[0], *weights)
        blocks = [w.reshape(2, 16, -1, w.shape[-1]) for w in weights]
        count = float(sum(w.size for w in weights))
        out = put_out(update(count, gg, gd, blocks, m, v))
        return (*(o.reshape(w.shape) for o, w in zip(out[:3], weights)), *out[3:])

    whole, rows = P(None, None, None), P(None, "dp", None)
    return jax.shard_map(
        body,
        mesh=mesh,
        in_specs=(P(("rep", "dp"), None, None),) * 2 + (whole,) * 3 + (rows,) * 6,
        out_specs=(P("rep", None, None),) * 3 + (P("rep", "dp", None),) * 6,
        check_vma=False,
    )
```

```python
import functools

import jax
import jax.numpy as jnp
from jax import lax
from jax.experimental import pallas as pl
from jax.experimental.pallas import tpu as pltpu
from jax.sharding import PartitionSpec as P

F32, BF16 = jnp.float32, jnp.bfloat16
MESH = pl.DeviceIdType.MESH

T, D, FF = 2048, 640, 2560
F = 256
TILES = FF // F
R = 512
STEPS = T // R
PIECE = 64
DEPTH = 4
UP, DOWN = 4, 3
HOPS = UP + DOWN
ROUNDS = UP + 1
L0 = TILES + 2
LAST = L0 + TILES


def ring(p):
    return p + (p // 4) * (11 - 2 * p)


def dot(a, b):
    return jnp.dot(a, b, preferred_element_type=F32)


def dot_nt(a, b):
    return lax.dot_general(a, b, (((1,), (1,)), ((), ())), preferred_element_type=F32)


def dot_tn(a, b):
    return lax.dot_general(a, b, (((0,), (0,)), ((), ())), preferred_element_type=F32)


def sigmoid(x):
    return jax.nn.sigmoid(x)


def scale_of(wide):
    return lax.rsqrt(jnp.mean(wide * wide, -1, keepdims=True) + 1e-6)


def where_am_i():
    rep, dp = lax.axis_index("rep"), lax.axis_index("dp")
    chip, core = dp // 2, dp % 2
    way = 1 - 2 * core
    return rep, dp, chip, core, way, ring(chip)


def remote(src, dst, send, recv, rep, device):
    return pltpu.make_async_remote_copy(
        src_ref=src, dst_ref=dst, send_sem=send, recv_sem=recv, device_id=(rep, device), device_id_type=MESH)


def grad_kernel(x_hbm, dy_hbm, wg_hbm, wu_hbm, wd_hbm,
                gg_hbm, gd_hbm, gu_hbm, hid_hbm,
                h, a, a0t, a1t, dy, acc, hid, dg, du, wg, wu, wd, gu,
                own, other, hop, ownd, otherd, hopd, gg, gd,
                io_sem, w_sem, gu_sem, hid_sem,
                half_send, half_recv, hop_send, hop_recv, dhalf_send, dhalf_recv, dhop_send, dhop_recv):
    rep, dp, chip, core, way, place = where_am_i()
    to = 2 * ring((place + way + 8) % 8) + core
    back = 2 * ring((place - way + 8) % 8) + core
    partner = dp + way

    barrier = pltpu.get_barrier_semaphore()
    for device in (to, back, partner):
        pl.semaphore_signal(barrier, inc=1, device_id=(rep, device), device_id_type=MESH)

    x_copy = pltpu.make_async_copy(x_hbm, h, io_sem.at[0])
    dy_copy = pltpu.make_async_copy(dy_hbm, dy, io_sem.at[1])
    x_copy.start()

    def cols(j):
        return pl.ds(pl.multiple_of(j * F, F), F)

    def rows(t):
        return pl.ds(t * R, R) if isinstance(t, int) else pl.ds(pl.multiple_of(t * R, R), R)

    def w_copies(k):
        layer, j, slot = (k // TILES) % 2, k % TILES, k % 2
        return (
            pltpu.make_async_copy(wg_hbm.at[layer, :, cols(j)], wg.at[slot], w_sem.at[0, slot]),
            pltpu.make_async_copy(wu_hbm.at[layer, :, cols(j)], wu.at[slot], w_sem.at[1, slot]),
            pltpu.make_async_copy(wd_hbm.at[layer, cols(j), :], wd.at[slot], w_sem.at[2, slot]),
        )

    def w_start(k):
        for c in w_copies(k):
            c.start()

    def w_wait(k):
        for c in w_copies(k):
            c.wait()

    def gu_copies(k, out):
        j, t, slot = k // STEPS, k % STEPS, k % DEPTH
        for n in range(2):
            there, here = gu_hbm.at[n, j, rows(t), :], gu.at[slot, n]
            yield pltpu.make_async_copy(here, there, gu_sem.at[n, slot]) if out else pltpu.make_async_copy(
                there, here, gu_sem.at[n, slot])

    def hid_copy(j, out):
        there, here = hid_hbm.at[j], hid.at[j % 3]
        return (pltpu.make_async_copy(here, there, hid_sem.at[j % 3]) if out
                else pltpu.make_async_copy(there, here, hid_sem.at[j % 3]))

    w_start(0)
    x_copy.wait()
    dy_copy.start()

    def ahead(s):
        return (place + way * (UP - s) + 16) % 8

    def behind(s):
        return (place - way * (DOWN - s) + 16) % 8

    def half(i):
        return remote(own.at[i % TILES, :, 1 - core], other.at[i], half_send.at[i], half_recv.at[i], rep, partner)

    def hop_copy(i, slot, src):
        return remote(src, hop.at[i, slot], hop_send.at[i, slot], hop_recv.at[i, slot], rep, to if slot < UP else back)

    def added(i, who):
        return own.at[i % TILES, who, core][...].astype(F32) + other.at[i, who][...].astype(F32)

    def half_d(d, who):
        rows_ = pl.ds(pl.multiple_of((2 * who + 1 - core) * 160, 32), 160)
        return remote(ownd.at[d, rows_], otherd.at[d, who], dhalf_send.at[d, who], dhalf_recv.at[d, who], rep, partner)

    def hop_copy_d(d, slot, src, device):
        return remote(src, hopd.at[d, slot], dhop_send.at[d, slot], dhop_recv.at[d, slot], rep, device)

    def rows_d(who):
        return pl.ds(pl.multiple_of((2 * who + core) * 160, 32), 160)

    def added_d(d, who):
        half_d(d, who).wait_recv()
        return ownd.at[d, rows_d(who)][...].astype(F32) + otherd.at[d, who][...].astype(F32)

    def serve(n):
        for age in range(1, ROUNDS + 1):
            c = n - age
            late = jnp.where(c >= L0, 1, 0)
            i = c - 2 * late

            @pl.when(((c >= 0) & (c < TILES)) | ((c >= L0) & (c < LAST)))
            def _():
                s = age - 1
                if s == 0:
                    half(i).wait_recv()
                    for slot, p in ((0, ahead(0)), (UP, behind(0))):
                        mine = own.at[i % TILES, ring(p), core]
                        mine[...] = added(i, ring(p)).astype(BF16)
                        hop_copy(i, slot, mine).start()
                elif s < UP:
                    for slot, p in ((s, ahead(s)), (UP + s, behind(s)))[: 2 if s < DOWN else 1]:
                        before = hop.at[i, slot - 1]
                        hop_copy(i, slot - 1, before).wait_recv()
                        before[...] = (before[...].astype(F32) + added(i, ring(p))).astype(BF16)
                        hop_copy(i, slot, before).start()
                else:
                    one, two = hop.at[i, UP - 1], hop.at[i, HOPS - 1]
                    hop_copy(i, UP - 1, one).wait_recv()
                    hop_copy(i, HOPS - 1, two).wait_recv()
                    new = (one[...].astype(F32) + two[...].astype(F32) + added(i, chip)).astype(BF16)
                    gg.at[1 - late][:, :, cols(i % TILES)] = new
                    half(i).wait_send()
                    for r in range(HOPS):
                        hop_copy(i, r, one).wait_send()

    def quarter(p):
        t = p // 2
        return t + (t // 2) * (5 - 2 * t)

    def ready(q):
        return (5 * (q + 1) - 1) // 2

    def serve_d(d, q, age):
        s = age - 1
        for base, hops, place_of, device in ((0, UP, ahead, to), (UP, DOWN, behind, back)):
            p = place_of(s)
            here = quarter(p) == q

            @pl.when((s == 0) & here)
            def _():
                mine = ownd.at[d, rows_d(ring(p))]
                mine[...] = added_d(d, ring(p)).astype(BF16)
                hop_copy_d(d, base, mine, device).start()

            @pl.when((s > 0) & (s < hops) & here)
            def _():
                before = hopd.at[d, base + s - 1]
                hop_copy_d(d, base + s - 1, before, device).wait_recv()
                before[...] = (before[...].astype(F32) + added_d(d, ring(p))).astype(BF16)
                hop_copy_d(d, base + s, before, device).start()

        @pl.when((s == UP) & (quarter(place) == q))
        def _():
            one, two = hopd.at[d, UP - 1], hopd.at[d, HOPS - 1]
            hop_copy_d(d, UP - 1, one, to).wait_recv()
            hop_copy_d(d, HOPS - 1, two, back).wait_recv()
            gd.at[d][...] = (one[...].astype(F32) + two[...].astype(F32) + added_d(d, chip)).astype(BF16)

    def put(i, n, t_, grad):
        g = dot(t_[...], grad[...]).astype(BF16)
        for o in range(16):
            own.at[i % TILES, o // 2, o % 2, n][...] = g[40 * o : 40 * o + 40]

    def pieces(t):
        for i in range(0, R, PIECE):
            at = t * R + i
            yield slice(i, i + PIECE), pl.ds(at if isinstance(t, int) else pl.multiple_of(at, PIECE), PIECE)

    def norm(t, to_t):
        wide = h[rows(t), :].astype(F32)
        one = (wide * scale_of(wide)).astype(BF16)
        a[rows(t), :] = one
        to_t[:, rows(t)] = one.T
        acc[rows(t), :] = jnp.zeros((R, D), F32)

    def first(t, z):
        norm(t, a0t)
        return z

    lax.fori_loop(0, STEPS, first, 0)

    hid.at[2][rows(STEPS - 1), :] = jnp.zeros((R, F), BF16)
    wd.at[1][...] = jnp.zeros((F, D), BF16)

    def forward(j, z):
        w_wait(j)

        @pl.when(j >= 3)
        def _():
            hid_copy(j - 3, True).wait()

        def step(t, before):
            k = j * STEPS + t
            h_slot, w_slot, t_before = before
            acc[rows(t_before), :] += dot(hid[h_slot, rows(t_before), :], wd[w_slot])
            gate, up = dot(a[rows(t), :], wg[j % 2]), dot(a[rows(t), :], wu[j % 2])

            @pl.when(k >= DEPTH)
            def _():
                for c in gu_copies(k - DEPTH, True):
                    c.wait()

            for here, there in pieces(t):
                one, two = gate[here], up[here]
                gu.at[k % DEPTH, 0][here, :] = one
                gu.at[k % DEPTH, 1][here, :] = two
                hid.at[j % 3][there, :] = (one * sigmoid(one) * two).astype(BF16)
            for c in gu_copies(k, True):
                c.start()

        step(0, ((j + 2) % 3, (j + 1) % 2, STEPS - 1))
        w_start(j + 1)
        for t in range(1, STEPS):
            step(t, (j % 3, j % 2, t - 1))
        hid_copy(j, True).start()
        return z

    lax.fori_loop(0, TILES, forward, 0)
    acc[rows(STEPS - 1), :] += dot(hid[(TILES - 1) % 3, rows(STEPS - 1), :], wd[(TILES - 1) % 2])
    for k in range(TILES * STEPS - DEPTH, TILES * STEPS):
        for c in gu_copies(k, True):
            c.wait()
    for j in range(TILES - 3, TILES):
        hid_copy(j, True).wait()

    def second(t, z):
        h[rows(t), :] = (h[rows(t), :].astype(F32) + acc[rows(t), :].astype(BF16).astype(F32)).astype(BF16)
        norm(t, a1t)
        return z

    lax.fori_loop(0, STEPS, second, 0)
    dy_copy.wait()
    pl.semaphore_wait(barrier, 3)

    def back_of(gate, up, by_hidden, there, to_hidden=None):
        sig = sigmoid(gate)
        silu = gate * sig
        dg[there, :] = (by_hidden * up * (sig + silu * (1.0 - sig))).astype(BF16)
        du[there, :] = (by_hidden * silu).astype(BF16)
        if to_hidden is not None:
            to_hidden[there, :] = (silu * up).astype(BF16)

    def tile(j, z):
        k = TILES + j
        slot = k % 2
        w_wait(k)
        w_start(k + 1)

        def step(t, z):
            gate, up = dot(a[rows(t), :], wg[slot]), dot(a[rows(t), :], wu[slot])
            by_hidden = dot_nt(dy[rows(t), :], wd[slot]).astype(BF16).astype(F32)
            for here, there in pieces(t):
                back_of(gate[here], up[here], by_hidden[here], there, hid.at[0])
            return z

        for t in range(STEPS):
            step(t, 0)
        serve(j)

        def quarters(q, z):
            serve_d(1, q, j - ready(q))
            return z

        lax.fori_loop(0, 3, quarters, 0)
        put(j, 0, a1t, dg)
        put(j, 1, a1t, du)
        half(j).start()
        ownd.at[1][cols(j), :] = dot_tn(hid[0], dy[...]).astype(BF16)

        for q in range(4):
            @pl.when(j == ready(q))
            def _():
                half_d(1, 2 * q).start()
                half_d(1, 2 * q + 1).start()


        def step_a(t, z):
            acc[rows(t), :] += dot_nt(dg[rows(t), :], wg[slot]) + dot_nt(du[rows(t), :], wu[slot])
            return z

        @pl.when(j == 0)
        def _():
            def clear(t, z):
                acc[rows(t), :] = jnp.zeros((R, D), F32)
                return z
            lax.fori_loop(0, STEPS, clear, 0)

        lax.fori_loop(0, STEPS, step_a, 0)
        return z

    lax.fori_loop(0, TILES, tile, 0)
    hid_copy(0, False).start()
    hid_copy(1, False).start()
    for k in range(DEPTH - 1):
        for c in gu_copies(k, False):
            c.start()

    def by_h(t, z):
        by_a = acc[rows(t), :].astype(BF16).astype(F32)
        wide = h[rows(t), :].astype(F32)
        scale = scale_of(wide)
        by_wide = scale * by_a - wide * (scale * scale * scale * jnp.mean(by_a * wide, -1, keepdims=True))
        dy[rows(t), :] = (dy[rows(t), :].astype(F32) + by_wide.astype(BF16).astype(F32)).astype(BF16)
        return z

    lax.fori_loop(0, STEPS, by_h, 0)

    def down(r, z):
        def one(jj, z):
            j = r * (TILES // 2) + jj
            hid_copy(j, False).wait()

            @pl.when(j + 2 < TILES)
            def _():
                hid_copy(j + 2, False).start()

            ownd.at[0][cols(j), :] = dot_tn(hid[j % 3], dy[...]).astype(BF16)
            return z

        lax.fori_loop(0, TILES // 2, one, 0)
        for i in range(4):
            half_d(0, 4 * r + i).start()
        serve(TILES + r)

        def quarters(q, z):
            serve_d(1, q, TILES + r - ready(q))
            serve_d(0, q, r - q // 2)
            return z

        lax.fori_loop(0, 4, quarters, 0)
        return z

    lax.fori_loop(0, 2, down, 0)

    def wd_copy(k):
        return pltpu.make_async_copy(wd_hbm.at[0, cols(k % TILES), :], wd.at[k % 2], w_sem.at[2, k % 2])

    w_wait(2 * TILES)
    wd_copy(2 * TILES + 1).start()

    def by_hidden(t, z):
        hid.at[0][rows(t), :] = dot_nt(dy[rows(t), :], wd[0]).astype(BF16)
        return z

    lax.fori_loop(0, STEPS, by_hidden, 0)

    def tile0(j, z):
        k = 2 * TILES + j

        @pl.when(j + 1 < TILES)
        def _():
            wd_copy(k + 1).wait()

        @pl.when(j + 2 < TILES)
        def _():
            wd_copy(k + 2).start()

        def step(t, z):
            n = j * STEPS + t
            for c in gu_copies(n, False):
                c.wait()

            @pl.when(n + DEPTH - 1 < TILES * STEPS)
            def _():
                for c in gu_copies(n + DEPTH - 1, False):
                    c.start()

            hid.at[(j + 1) % 2][rows(t), :] = dot_nt(dy[rows(t), :], wd[(j + 1) % 2]).astype(BF16)
            for here, there in pieces(t):
                back_of(gu[n % DEPTH, 0, here, :], gu[n % DEPTH, 1, here, :], hid[j % 2, there, :].astype(F32), there)
            return z

        lax.fori_loop(0, STEPS, step, 0)
        serve(L0 + j)

        def quarters(q, z):
            serve_d(1, q, L0 + j - ready(q))
            serve_d(0, q, 2 + j - q // 2)
            return z

        lax.fori_loop(0, 4, quarters, 0)
        put(TILES + j, 0, a0t, dg)
        put(TILES + j, 1, a0t, du)
        half(TILES + j).start()
        return z

    lax.fori_loop(0, TILES, tile0, 0)

    def drain(r, z):
        serve(LAST + r)
        return z

    lax.fori_loop(0, ROUNDS, drain, 0)
    for d in range(2):
        for who in range(8):
            half_d(d, who).wait_send()
        for slot in range(HOPS):
            hop_copy_d(d, slot, hopd.at[d, slot], to).wait_send()
    out = [pltpu.make_async_copy(gg, gg_hbm, io_sem.at[0]), pltpu.make_async_copy(gd, gd_hbm, io_sem.at[1])]
    for c in out:
        c.start()
    for c in out:
        c.wait()


def grads(x, dy, wg, wu, wd):
    any_ = pl.BlockSpec(memory_space=pl.ANY)
    dma, vmem = pltpu.SemaphoreType.DMA, pltpu.VMEM
    s = jax.ShapeDtypeStruct
    block = (2, 40, F)
    out = pl.pallas_call(
        grad_kernel,
        out_shape=[s((2, 2, 40, FF), BF16), s((2, 160, D), BF16),
                   s((2, TILES, T, F), F32), s((TILES, T, F), BF16)],
        in_specs=[any_] * 5,
        out_specs=[any_] * 4,
        scratch_shapes=[
            vmem((T, D), BF16), vmem((T, D), BF16), vmem((D, T), BF16), vmem((D, T), BF16), vmem((T, D), BF16),
            vmem((T, D), F32), vmem((3, T, F), BF16), vmem((T, F), BF16), vmem((T, F), BF16),
            vmem((2, D, F), BF16), vmem((2, D, F), BF16), vmem((2, F, D), BF16), vmem((DEPTH, 2, R, F), F32),
            vmem((TILES, 8, 2, *block), BF16), vmem((2 * TILES, 8, *block), BF16), vmem((2 * TILES, HOPS, *block), BF16),
            vmem((2, FF, D), BF16), vmem((2, 8, 160, D), BF16), vmem((2, HOPS, 160, D), BF16),
            vmem((2, 2, 40, FF), BF16), vmem((2, 160, D), BF16),
            dma((2,)), dma((3, 2)), dma((2, DEPTH)), dma((3,)),
            dma((2 * TILES,)), dma((2 * TILES,)), dma((2 * TILES, HOPS)), dma((2 * TILES, HOPS)),
            dma((2, 8)), dma((2, 8)), dma((2, HOPS)), dma((2, HOPS)),
        ],
        compiler_params=pltpu.CompilerParams(
            collective_id=1, has_side_effects=True, vmem_limit_bytes=67043328),
    )(x, dy, wg, wu, wd)
    return out[:2]


def update_kernel(count, *refs):
    gg_hbm, gd_hbm, w, m, v = refs[0], refs[1], refs[2:5], refs[5:8], refs[8:11]
    w_out, m_out, v_out = refs[11:14], refs[14:17], refs[17:20]
    (gg, gd, mg, md, vg, vd, wg, wd, sums, g_sem, load_sem, sum_send, sum_recv,
     ag_send, ag_recv, d2d_send, d2d_recv, store_sem) = refs[20:]
    items = [(0, 0), (1, 0), (2, 0), (0, 1), (1, 1), (2, 1)]

    def at(k, big, small):
        which, layer_ = items[k]
        return small.at[layer_] if which == 2 else big.at[layer_, which]

    rep, dp, chip, core, way, place = where_am_i()
    to = 2 * ring((place + way + 8) % 8) + core
    partner = dp + way

    barrier = pltpu.get_barrier_semaphore()
    for off in range(1, 16):
        pl.semaphore_signal(barrier, inc=1, device_id=(rep, (dp + off) % 16), device_id_type=MESH)

    g_loads = [pltpu.make_async_copy(gg_hbm, gg, g_sem.at[0]), pltpu.make_async_copy(gd_hbm, gd, g_sem.at[1])]
    for c in g_loads:
        c.start()
    loads = []
    for k, (which, layer_) in enumerate(items):
        for n, (src, dst) in enumerate((
            (m[which].at[layer_], at(k, mg, md)),
            (v[which].at[layer_], at(k, vg, vd)),
            (w[which].at[layer_, dp], at(k, wg, wd)),
        )):
            c = pltpu.make_async_copy(src, dst, load_sem.at[k, n])
            c.start()
            loads.append(c)
    for c in g_loads:
        c.wait()

    squares = jnp.zeros((8, 128), F32)
    for k in range(6):
        g = at(k, gg, gd)[...].astype(F32)
        g = g * g
        part = g[0:8]
        for i in range(1, g.shape[0] // 8):
            part = part + g[8 * i : 8 * i + 8]
        for i in range(part.shape[1] // 128):
            squares = squares + part[:, 128 * i : 128 * i + 128]
    sums.at[dp][...] = squares
    pl.semaphore_wait(barrier, 15)

    def sum_copy(off):
        return remote(sums.at[dp], sums.at[dp], sum_send.at[off], sum_recv.at[off], rep, (dp + off) % 16)

    for off in range(1, 16):
        sum_copy(off).start()
    for c in loads:
        c.wait()
    for off in range(1, 16):
        sum_copy(off).wait_recv()
    mean = jnp.sum(sums[...]) / count
    factor = jnp.minimum(1.0, 0.5 * lax.rsqrt(jnp.full((8, 128), mean + 1e-30, F32)))[0:1, 0:1]

    def block(k, who):
        which, layer_ = items[k]
        return w_out[which].at[layer_, who]

    def gather_copy(k, s, who, src=None):
        src = block(k, who) if src is None else src
        return remote(src, block(k, who), ag_send.at[k, s], ag_recv.at[k, s], rep, to)

    def d2d_copy(k, s, who, src=None):
        src = block(k, who) if src is None else src
        return remote(src, block(k, who), d2d_send.at[k, s], d2d_recv.at[k, s], rep, partner)

    stores = []
    for k, (which, layer_) in enumerate(items):
        g = at(k, gg, gd)[...].astype(F32) * factor
        mk, vk, wk = at(k, mg, md), at(k, vg, vd), at(k, wg, wd)
        new_m = 0.9 * mk[...] + 0.1 * g
        new_v = 0.95 * vk[...] + 0.05 * g * g
        wide = wk[...].astype(F32)
        wk[...] = (wide - 0.02 * (new_m * lax.rsqrt(new_v + 1e-8) + 0.1 * wide)).astype(BF16)
        mk[...] = new_m
        vk[...] = new_v
        gather_copy(k, 0, dp, wk).start()
        d2d_copy(k, 0, dp, wk).start()
        for n, (src, dst) in enumerate((
            (wk, block(k, dp)), (mk, m_out[which].at[layer_]), (vk, v_out[which].at[layer_]))):
            c = pltpu.make_async_copy(src, dst, store_sem.at[k, n])
            c.start()
            stores.append(c)

    def source(s):
        return 2 * ring((place - way * (1 + s) + 16) % 8) + core

    def gather(s, z):
        for k in range(6):
            who = source(s)
            gather_copy(k, s, who).wait_recv()
            gather_copy(k, s + 1, who).start()
            d2d_copy(k, s + 1, who).start()
        return z

    lax.fori_loop(0, 6, gather, 0)
    for k in range(6):
        who = source(6)
        gather_copy(k, 6, who).wait_recv()
        d2d_copy(k, 7, who).start()

    for c in stores:
        c.wait()
    for off in range(1, 16):
        sum_copy(off).wait_send()

    def drain(s, z):
        for k in range(6):
            gather_copy(k, s, dp).wait_send()
            d2d_copy(k, s, dp).wait_send()
            d2d_copy(k, s, dp).wait_recv()
        return z

    lax.fori_loop(0, 7, drain, 0)
    for k in range(6):
        d2d_copy(k, 7, dp).wait_send()
        d2d_copy(k, 7, dp).wait_recv()


def update(count, gg, gd, weights, m, v):
    G, S = (2, 2, 40, FF), (2, 160, D)
    any_ = pl.BlockSpec(memory_space=pl.ANY)
    dma, vmem = pltpu.SemaphoreType.DMA, pltpu.VMEM
    return pl.pallas_call(
        functools.partial(update_kernel, count),
        out_shape=[
            *(jax.ShapeDtypeStruct(t.shape, BF16) for t in weights),
            *(jax.ShapeDtypeStruct(t.shape, F32) for t in (*m, *v)),
        ],
        in_specs=[pl.BlockSpec(memory_space=pltpu.HBM)] * 11,
        out_specs=[any_] * 9,
        scratch_shapes=[
            vmem(G, BF16), vmem(S, BF16), vmem(G, F32), vmem(S, F32), vmem(G, F32), vmem(S, F32), vmem(G, BF16), vmem(S, BF16),
            vmem((16, 8, 128), F32),
            dma((2,)), dma((6, 3)), dma((16,)), dma((16,)),
            dma((6, 7)), dma((6, 7)), dma((6, 8)), dma((6, 8)), dma((6, 3)),
        ],
        compiler_params=pltpu.CompilerParams(
            collective_id=0, has_side_effects=True, vmem_limit_bytes=16 * 1024 * 1024),
    )(*(pltpu.with_memory_space_constraint(t, pltpu.HBM) for t in (gg, gd, *weights, *m, *v)))


def out_kernel(n, *refs):
    copies = [pltpu.make_async_copy(refs[i], refs[n + i], refs[2 * n].at[i]) for i in range(n)]
    for c in copies:
        c.start()
    for c in copies:
        c.wait()


def put_out(arrays):
    n = len(arrays)
    return pl.pallas_call(
        functools.partial(out_kernel, n),
        out_shape=[jax.ShapeDtypeStruct(t.shape, t.dtype) for t in arrays],
        in_specs=[pl.BlockSpec(memory_space=pl.ANY)] * n,
        out_specs=[pl.BlockSpec(memory_space=pltpu.HBM)] * n,
        scratch_shapes=[pltpu.SemaphoreType.DMA((n,))],
        compiler_params=pltpu.CompilerParams(vmem_limit_bytes=1024 * 1024),
    )(*arrays)


def solution(mesh):
    def body(x, dy, *arrays):
        weights, m, v = (arrays[i : i + 3] for i in (0, 3, 6))
        gg, gd = grads(x[0], dy[0], *weights)
        blocks = [w.reshape(2, 16, -1, w.shape[-1]) for w in weights]
        count = float(sum(w.size for w in weights))
        out = put_out(update(count, gg, gd, blocks, m, v))
        return (*(o.reshape(w.shape) for o, w in zip(out[:3], weights)), *out[3:])

    whole, rows = P(None, None, None), P(None, "dp", None)
    return jax.shard_map(
        body,
        mesh=mesh,
        in_specs=(P(("rep", "dp"), None, None),) * 2 + (whole,) * 3 + (rows,) * 6,
        out_specs=(P("rep", None, None),) * 3 + (P("rep", "dp", None),) * 6,
        check_vma=False,
    )
```

```python
import functools

import jax
import jax.numpy as jnp
from jax import lax
from jax.experimental import pallas as pl
from jax.experimental.pallas import tpu as pltpu
from jax.sharding import PartitionSpec as P

F32, BF16 = jnp.float32, jnp.bfloat16
MESH = pl.DeviceIdType.MESH

T, D, FF = 2048, 640, 2560
F = 256
TILES = FF // F
R = 512
STEPS = T // R
PIECE = 64
DEPTH = 4
UP, DOWN = 4, 3
HOPS = UP + DOWN
ROUNDS = UP + 1
L0 = TILES + 2
LAST = L0 + TILES


def ring(p):
    return p + (p // 4) * (11 - 2 * p)


def dot(a, b):
    return jnp.dot(a, b, preferred_element_type=F32)


def dot_nt(a, b):
    return lax.dot_general(a, b, (((1,), (1,)), ((), ())), preferred_element_type=F32)


def dot_tn(a, b):
    return lax.dot_general(a, b, (((0,), (0,)), ((), ())), preferred_element_type=F32)


def sigmoid(x):
    return jax.nn.sigmoid(x)


def scale_of(wide):
    return lax.rsqrt(jnp.mean(wide * wide, -1, keepdims=True) + 1e-6)


def where_am_i():
    rep, dp = lax.axis_index("rep"), lax.axis_index("dp")
    chip, core = dp // 2, dp % 2
    way = 1 - 2 * core
    return rep, dp, chip, core, way, ring(chip)


def remote(src, dst, send, recv, rep, device):
    return pltpu.make_async_remote_copy(
        src_ref=src, dst_ref=dst, send_sem=send, recv_sem=recv, device_id=(rep, device), device_id_type=MESH)


def grad_kernel(x_hbm, dy_hbm, wg_hbm, wu_hbm, wd_hbm,
                gg_hbm, gd_hbm, gu_hbm, hid_hbm,
                h, a, a0t, a1t, dy, acc, hid, dg, du, wg, wu, wd, wgt, wut, wdt, gu,
                own, other, hop, ownd, otherd, hopd, gg, gd,
                io_sem, w_sem, gu_sem, hid_sem,
                half_send, half_recv, hop_send, hop_recv, dhalf_send, dhalf_recv, dhop_send, dhop_recv):
    rep, dp, chip, core, way, place = where_am_i()
    to = 2 * ring((place + way + 8) % 8) + core
    back = 2 * ring((place - way + 8) % 8) + core
    partner = dp + way

    barrier = pltpu.get_barrier_semaphore()
    for device in (to, back, partner):
        pl.semaphore_signal(barrier, inc=1, device_id=(rep, device), device_id_type=MESH)

    x_copy = pltpu.make_async_copy(x_hbm, h, io_sem.at[0])
    dy_copy = pltpu.make_async_copy(dy_hbm, dy, io_sem.at[1])
    x_copy.start()

    def cols(j):
        return pl.ds(pl.multiple_of(j * F, F), F)

    def rows(t):
        return pl.ds(t * R, R) if isinstance(t, int) else pl.ds(pl.multiple_of(t * R, R), R)

    def w_copies(k):
        layer, j, slot = (k // TILES) % 2, k % TILES, k % 2
        return (
            pltpu.make_async_copy(wg_hbm.at[layer, :, cols(j)], wg.at[slot], w_sem.at[0, slot]),
            pltpu.make_async_copy(wu_hbm.at[layer, :, cols(j)], wu.at[slot], w_sem.at[1, slot]),
            pltpu.make_async_copy(wd_hbm.at[layer, cols(j), :], wd.at[slot], w_sem.at[2, slot]),
        )

    def w_start(k):
        for c in w_copies(k):
            c.start()

    def w_wait(k):
        for c in w_copies(k):
            c.wait()

    def gu_copies(k, out):
        j, t, slot = k // STEPS, k % STEPS, k % DEPTH
        for n in range(2):
            there, here = gu_hbm.at[n, j, rows(t), :], gu.at[slot, n]
            yield pltpu.make_async_copy(here, there, gu_sem.at[n, slot]) if out else pltpu.make_async_copy(
                there, here, gu_sem.at[n, slot])

    def hid_copy(j, out):
        there, here = hid_hbm.at[j], hid.at[j % 3]
        return (pltpu.make_async_copy(here, there, hid_sem.at[j % 3]) if out
                else pltpu.make_async_copy(there, here, hid_sem.at[j % 3]))

    w_start(0)
    x_copy.wait()
    dy_copy.start()

    def ahead(s):
        return (place + way * (UP - s) + 16) % 8

    def behind(s):
        return (place - way * (DOWN - s) + 16) % 8

    def half(i):
        return remote(own.at[i % TILES, :, 1 - core], other.at[i], half_send.at[i], half_recv.at[i], rep, partner)

    def hop_copy(i, slot, src):
        return remote(src, hop.at[i, slot], hop_send.at[i, slot], hop_recv.at[i, slot], rep, to if slot < UP else back)

    def added(i, who):
        return own.at[i % TILES, who, core][...].astype(F32) + other.at[i, who][...].astype(F32)

    def half_d(d, who):
        rows_ = pl.ds(pl.multiple_of((2 * who + 1 - core) * 160, 32), 160)
        return remote(ownd.at[d, rows_], otherd.at[d, who], dhalf_send.at[d, who], dhalf_recv.at[d, who], rep, partner)

    def hop_copy_d(d, slot, src, device):
        return remote(src, hopd.at[d, slot], dhop_send.at[d, slot], dhop_recv.at[d, slot], rep, device)

    def rows_d(who):
        return pl.ds(pl.multiple_of((2 * who + core) * 160, 32), 160)

    def added_d(d, who):
        half_d(d, who).wait_recv()
        return ownd.at[d, rows_d(who)][...].astype(F32) + otherd.at[d, who][...].astype(F32)

    def serve(n):
        for age in range(1, ROUNDS + 1):
            c = n - age
            late = jnp.where(c >= L0, 1, 0)
            i = c - 2 * late

            @pl.when(((c >= 0) & (c < TILES)) | ((c >= L0) & (c < LAST)))
            def _():
                s = age - 1
                if s == 0:
                    half(i).wait_recv()
                    for slot, p in ((0, ahead(0)), (UP, behind(0))):
                        mine = own.at[i % TILES, ring(p), core]
                        mine[...] = added(i, ring(p)).astype(BF16)
                        hop_copy(i, slot, mine).start()
                elif s < UP:
                    for slot, p in ((s, ahead(s)), (UP + s, behind(s)))[: 2 if s < DOWN else 1]:
                        before = hop.at[i, slot - 1]
                        hop_copy(i, slot - 1, before).wait_recv()
                        before[...] = (before[...].astype(F32) + added(i, ring(p))).astype(BF16)
                        hop_copy(i, slot, before).start()
                else:
                    one, two = hop.at[i, UP - 1], hop.at[i, HOPS - 1]
                    hop_copy(i, UP - 1, one).wait_recv()
                    hop_copy(i, HOPS - 1, two).wait_recv()
                    new = (one[...].astype(F32) + two[...].astype(F32) + added(i, chip)).astype(BF16)
                    gg.at[1 - late][:, :, cols(i % TILES)] = new
                    half(i).wait_send()
                    for r in range(HOPS):
                        hop_copy(i, r, one).wait_send()

    def quarter(p):
        t = p // 2
        return t + (t // 2) * (5 - 2 * t)

    def ready(q):
        return (5 * (q + 1) - 1) // 2

    def serve_d(d, q, age):
        s = age - 1
        for base, hops, place_of, device in ((0, UP, ahead, to), (UP, DOWN, behind, back)):
            p = place_of(s)
            here = quarter(p) == q

            @pl.when((s == 0) & here)
            def _():
                mine = ownd.at[d, rows_d(ring(p))]
                mine[...] = added_d(d, ring(p)).astype(BF16)
                hop_copy_d(d, base, mine, device).start()

            @pl.when((s > 0) & (s < hops) & here)
            def _():
                before = hopd.at[d, base + s - 1]
                hop_copy_d(d, base + s - 1, before, device).wait_recv()
                before[...] = (before[...].astype(F32) + added_d(d, ring(p))).astype(BF16)
                hop_copy_d(d, base + s, before, device).start()

        @pl.when((s == UP) & (quarter(place) == q))
        def _():
            one, two = hopd.at[d, UP - 1], hopd.at[d, HOPS - 1]
            hop_copy_d(d, UP - 1, one, to).wait_recv()
            hop_copy_d(d, HOPS - 1, two, back).wait_recv()
            gd.at[d][...] = (one[...].astype(F32) + two[...].astype(F32) + added_d(d, chip)).astype(BF16)

    def put(i, n, t_, grad):
        g = dot(t_[...], grad[...]).astype(BF16)
        for o in range(16):
            own.at[i % TILES, o // 2, o % 2, n][...] = g[40 * o : 40 * o + 40]

    def pieces(t):
        for i in range(0, R, PIECE):
            at = t * R + i
            yield slice(i, i + PIECE), pl.ds(at if isinstance(t, int) else pl.multiple_of(at, PIECE), PIECE)

    def norm(t, to_t):
        wide = h[rows(t), :].astype(F32)
        one = (wide * scale_of(wide)).astype(BF16)
        a[rows(t), :] = one
        to_t[:, rows(t)] = one.T
        acc[rows(t), :] = jnp.zeros((R, D), F32)

    def first(t, z):
        norm(t, a0t)
        return z

    lax.fori_loop(0, STEPS, first, 0)

    hid.at[2][rows(STEPS - 1), :] = jnp.zeros((R, F), BF16)
    wd.at[1][...] = jnp.zeros((F, D), BF16)

    def forward(j, z):
        w_wait(j)

        @pl.when(j >= 3)
        def _():
            hid_copy(j - 3, True).wait()

        def step(t, before):
            k = j * STEPS + t
            h_slot, w_slot, t_before = before
            acc[rows(t_before), :] += dot(hid[h_slot, rows(t_before), :], wd[w_slot])
            gate, up = dot(a[rows(t), :], wg[j % 2]), dot(a[rows(t), :], wu[j % 2])

            @pl.when(k >= DEPTH)
            def _():
                for c in gu_copies(k - DEPTH, True):
                    c.wait()

            for here, there in pieces(t):
                one, two = gate[here], up[here]
                gu.at[k % DEPTH, 0][here, :] = one
                gu.at[k % DEPTH, 1][here, :] = two
                hid.at[j % 3][there, :] = (one * sigmoid(one) * two).astype(BF16)
            for c in gu_copies(k, True):
                c.start()

        step(0, ((j + 2) % 3, (j + 1) % 2, STEPS - 1))
        w_start(j + 1)
        for t in range(1, STEPS):
            step(t, (j % 3, j % 2, t - 1))
        hid_copy(j, True).start()
        return z

    lax.fori_loop(0, TILES, forward, 0)
    acc[rows(STEPS - 1), :] += dot(hid[(TILES - 1) % 3, rows(STEPS - 1), :], wd[(TILES - 1) % 2])
    for k in range(TILES * STEPS - DEPTH, TILES * STEPS):
        for c in gu_copies(k, True):
            c.wait()
    for j in range(TILES - 3, TILES):
        hid_copy(j, True).wait()

    def second(t, z):
        h[rows(t), :] = (h[rows(t), :].astype(F32) + acc[rows(t), :].astype(BF16).astype(F32)).astype(BF16)
        norm(t, a1t)
        return z

    lax.fori_loop(0, STEPS, second, 0)
    dy_copy.wait()
    pl.semaphore_wait(barrier, 3)

    def back_of(gate, up, by_hidden, there, to_hidden=None):
        sig = sigmoid(gate)
        silu = gate * sig
        dg[there, :] = (by_hidden * up * (sig + silu * (1.0 - sig))).astype(BF16)
        du[there, :] = (by_hidden * silu).astype(BF16)
        if to_hidden is not None:
            to_hidden[there, :] = (silu * up).astype(BF16)

    def tile(j, z):
        k = TILES + j
        slot = k % 2
        w_wait(k)
        w_start(k + 1)

        def step(t, z):
            gate, up = dot(a[rows(t), :], wg[slot]), dot(a[rows(t), :], wu[slot])
            by_hidden = dot(dy[rows(t), :], wdt[...]).astype(BF16).astype(F32)
            for here, there in pieces(t):
                back_of(gate[here], up[here], by_hidden[here], there, hid.at[0])
            return z

        wdt[...] = wd[slot].T
        for t in range(STEPS):
            step(t, 0)
        serve(j)

        def quarters(q, z):
            serve_d(1, q, j - ready(q))
            return z

        lax.fori_loop(0, 3, quarters, 0)
        wgt[...] = wg[slot].T
        wut[...] = wu[slot].T
        put(j, 0, a1t, dg)
        put(j, 1, a1t, du)
        half(j).start()
        ownd.at[1][cols(j), :] = dot_tn(hid[0], dy[...]).astype(BF16)

        for q in range(4):
            @pl.when(j == ready(q))
            def _():
                half_d(1, 2 * q).start()
                half_d(1, 2 * q + 1).start()


        def step_a(t, z):
            acc[rows(t), :] += dot(dg[rows(t), :], wgt[...]) + dot(du[rows(t), :], wut[...])
            return z

        @pl.when(j == 0)
        def _():
            def clear(t, z):
                acc[rows(t), :] = jnp.zeros((R, D), F32)
                return z
            lax.fori_loop(0, STEPS, clear, 0)

        lax.fori_loop(0, STEPS, step_a, 0)
        return z

    lax.fori_loop(0, TILES, tile, 0)
    hid_copy(0, False).start()
    hid_copy(1, False).start()
    for k in range(DEPTH - 1):
        for c in gu_copies(k, False):
            c.start()

    def by_h(t, z):
        by_a = acc[rows(t), :].astype(BF16).astype(F32)
        wide = h[rows(t), :].astype(F32)
        scale = scale_of(wide)
        by_wide = scale * by_a - wide * (scale * scale * scale * jnp.mean(by_a * wide, -1, keepdims=True))
        dy[rows(t), :] = (dy[rows(t), :].astype(F32) + by_wide.astype(BF16).astype(F32)).astype(BF16)
        return z

    lax.fori_loop(0, STEPS, by_h, 0)

    def down(r, z):
        def one(jj, z):
            j = r * (TILES // 2) + jj
            hid_copy(j, False).wait()

            @pl.when(j + 2 < TILES)
            def _():
                hid_copy(j + 2, False).start()

            ownd.at[0][cols(j), :] = dot_tn(hid[j % 3], dy[...]).astype(BF16)
            return z

        lax.fori_loop(0, TILES // 2, one, 0)
        for i in range(4):
            half_d(0, 4 * r + i).start()
        serve(TILES + r)

        def quarters(q, z):
            serve_d(1, q, TILES + r - ready(q))
            serve_d(0, q, r - 2 * q)
            return z

        lax.fori_loop(0, 4, quarters, 0)
        return z

    lax.fori_loop(0, 2, down, 0)

    def wd_copy(k):
        return pltpu.make_async_copy(wd_hbm.at[0, cols(k % TILES), :], wd.at[k % 2], w_sem.at[2, k % 2])

    w_wait(2 * TILES)
    wd_copy(2 * TILES + 1).start()

    def by_hidden(t, z):
        hid.at[0][rows(t), :] = dot_nt(dy[rows(t), :], wd[0]).astype(BF16)
        return z

    lax.fori_loop(0, STEPS, by_hidden, 0)

    def tile0(j, z):
        k = 2 * TILES + j

        @pl.when(j + 1 < TILES)
        def _():
            wd_copy(k + 1).wait()

        @pl.when(j + 2 < TILES)
        def _():
            wd_copy(k + 2).start()

        def step(t, z):
            n = j * STEPS + t
            for c in gu_copies(n, False):
                c.wait()

            @pl.when(n + DEPTH - 1 < TILES * STEPS)
            def _():
                for c in gu_copies(n + DEPTH - 1, False):
                    c.start()

            hid.at[(j + 1) % 2][rows(t), :] = dot_nt(dy[rows(t), :], wd[(j + 1) % 2]).astype(BF16)
            for here, there in pieces(t):
                back_of(gu[n % DEPTH, 0, here, :], gu[n % DEPTH, 1, here, :], hid[j % 2, there, :].astype(F32), there)
            return z

        lax.fori_loop(0, STEPS, step, 0)
        serve(L0 + j)

        def quarters(q, z):
            serve_d(1, q, L0 + j - ready(q))
            serve_d(0, q, 2 + j - 2 * q)
            return z

        lax.fori_loop(0, 4, quarters, 0)
        put(TILES + j, 0, a0t, dg)
        put(TILES + j, 1, a0t, du)
        half(TILES + j).start()
        return z

    lax.fori_loop(0, TILES, tile0, 0)

    def drain(r, z):
        serve(LAST + r)
        return z

    lax.fori_loop(0, ROUNDS, drain, 0)
    for d in range(2):
        for who in range(8):
            half_d(d, who).wait_send()
        for slot in range(HOPS):
            hop_copy_d(d, slot, hopd.at[d, slot], to).wait_send()
    out = [pltpu.make_async_copy(gg, gg_hbm, io_sem.at[0]), pltpu.make_async_copy(gd, gd_hbm, io_sem.at[1])]
    for c in out:
        c.start()
    for c in out:
        c.wait()


def grads(x, dy, wg, wu, wd):
    any_ = pl.BlockSpec(memory_space=pl.ANY)
    dma, vmem = pltpu.SemaphoreType.DMA, pltpu.VMEM
    s = jax.ShapeDtypeStruct
    block = (2, 40, F)
    out = pl.pallas_call(
        grad_kernel,
        out_shape=[s((2, 2, 40, FF), BF16), s((2, 160, D), BF16),
                   s((2, TILES, T, F), F32), s((TILES, T, F), BF16)],
        in_specs=[any_] * 5,
        out_specs=[any_] * 4,
        scratch_shapes=[
            vmem((T, D), BF16), vmem((T, D), BF16), vmem((D, T), BF16), vmem((D, T), BF16), vmem((T, D), BF16),
            vmem((T, D), F32), vmem((3, T, F), BF16), vmem((T, F), BF16), vmem((T, F), BF16),
            vmem((2, D, F), BF16), vmem((2, D, F), BF16), vmem((2, F, D), BF16),
            vmem((F, D), BF16), vmem((F, D), BF16), vmem((D, F), BF16), vmem((DEPTH, 2, R, F), F32),
            vmem((TILES, 8, 2, *block), BF16), vmem((2 * TILES, 8, *block), BF16), vmem((2 * TILES, HOPS, *block), BF16),
            vmem((2, FF, D), BF16), vmem((2, 8, 160, D), BF16), vmem((2, HOPS, 160, D), BF16),
            vmem((2, 2, 40, FF), BF16), vmem((2, 160, D), BF16),
            dma((2,)), dma((3, 2)), dma((2, DEPTH)), dma((3,)),
            dma((2 * TILES,)), dma((2 * TILES,)), dma((2 * TILES, HOPS)), dma((2 * TILES, HOPS)),
            dma((2, 8)), dma((2, 8)), dma((2, HOPS)), dma((2, HOPS)),
        ],
        compiler_params=pltpu.CompilerParams(
            collective_id=1, has_side_effects=True, vmem_limit_bytes=67043328),
    )(x, dy, wg, wu, wd)
    return out[:2]


def update_kernel(count, *refs):
    gg_hbm, gd_hbm, w, m, v = refs[0], refs[1], refs[2:5], refs[5:8], refs[8:11]
    w_out, m_out, v_out = refs[11:14], refs[14:17], refs[17:20]
    (gg, gd, mg, md, vg, vd, wg, wd, sums, g_sem, load_sem, sum_send, sum_recv,
     ag_send, ag_recv, d2d_send, d2d_recv, store_sem) = refs[20:]
    items = [(0, 0), (1, 0), (2, 0), (0, 1), (1, 1), (2, 1)]

    def at(k, big, small):
        which, layer_ = items[k]
        return small.at[layer_] if which == 2 else big.at[layer_, which]

    rep, dp, chip, core, way, place = where_am_i()
    to = 2 * ring((place + way + 8) % 8) + core
    partner = dp + way

    barrier = pltpu.get_barrier_semaphore()
    for off in range(1, 16):
        pl.semaphore_signal(barrier, inc=1, device_id=(rep, (dp + off) % 16), device_id_type=MESH)

    g_loads = [pltpu.make_async_copy(gg_hbm, gg, g_sem.at[0]), pltpu.make_async_copy(gd_hbm, gd, g_sem.at[1])]
    for c in g_loads:
        c.start()
    loads = []
    for k, (which, layer_) in enumerate(items):
        for n, (src, dst) in enumerate((
            (m[which].at[layer_], at(k, mg, md)),
            (v[which].at[layer_], at(k, vg, vd)),
            (w[which].at[layer_, dp], at(k, wg, wd)),
        )):
            c = pltpu.make_async_copy(src, dst, load_sem.at[k, n])
            c.start()
            loads.append(c)
    for c in g_loads:
        c.wait()

    squares = jnp.zeros((8, 128), F32)
    for k in range(6):
        g = at(k, gg, gd)[...].astype(F32)
        g = g * g
        part = g[0:8]
        for i in range(1, g.shape[0] // 8):
            part = part + g[8 * i : 8 * i + 8]
        for i in range(part.shape[1] // 128):
            squares = squares + part[:, 128 * i : 128 * i + 128]
    sums.at[dp][...] = squares
    pl.semaphore_wait(barrier, 15)

    def sum_copy(off):
        return remote(sums.at[dp], sums.at[dp], sum_send.at[off], sum_recv.at[off], rep, (dp + off) % 16)

    for off in range(1, 16):
        sum_copy(off).start()
    for c in loads:
        c.wait()
    for off in range(1, 16):
        sum_copy(off).wait_recv()
    mean = jnp.sum(sums[...]) / count
    factor = jnp.minimum(1.0, 0.5 * lax.rsqrt(jnp.full((8, 128), mean + 1e-30, F32)))[0:1, 0:1]

    def block(k, who):
        which, layer_ = items[k]
        return w_out[which].at[layer_, who]

    def gather_copy(k, s, who, src=None):
        src = block(k, who) if src is None else src
        return remote(src, block(k, who), ag_send.at[k, s], ag_recv.at[k, s], rep, to)

    def d2d_copy(k, s, who, src=None):
        src = block(k, who) if src is None else src
        return remote(src, block(k, who), d2d_send.at[k, s], d2d_recv.at[k, s], rep, partner)

    stores = []
    for k, (which, layer_) in enumerate(items):
        g = at(k, gg, gd)[...].astype(F32) * factor
        mk, vk, wk = at(k, mg, md), at(k, vg, vd), at(k, wg, wd)
        new_m = 0.9 * mk[...] + 0.1 * g
        new_v = 0.95 * vk[...] + 0.05 * g * g
        wide = wk[...].astype(F32)
        wk[...] = (wide - 0.02 * (new_m * lax.rsqrt(new_v + 1e-8) + 0.1 * wide)).astype(BF16)
        mk[...] = new_m
        vk[...] = new_v
        gather_copy(k, 0, dp, wk).start()
        d2d_copy(k, 0, dp, wk).start()
        for n, (src, dst) in enumerate((
            (wk, block(k, dp)), (mk, m_out[which].at[layer_]), (vk, v_out[which].at[layer_]))):
            c = pltpu.make_async_copy(src, dst, store_sem.at[k, n])
            c.start()
            stores.append(c)

    def source(s):
        return 2 * ring((place - way * (1 + s) + 16) % 8) + core

    def gather(s, z):
        for k in range(6):
            who = source(s)
            gather_copy(k, s, who).wait_recv()
            gather_copy(k, s + 1, who).start()
            d2d_copy(k, s + 1, who).start()
        return z

    lax.fori_loop(0, 6, gather, 0)
    for k in range(6):
        who = source(6)
        gather_copy(k, 6, who).wait_recv()
        d2d_copy(k, 7, who).start()

    for c in stores:
        c.wait()
    for off in range(1, 16):
        sum_copy(off).wait_send()

    def drain(s, z):
        for k in range(6):
            gather_copy(k, s, dp).wait_send()
            d2d_copy(k, s, dp).wait_send()
            d2d_copy(k, s, dp).wait_recv()
        return z

    lax.fori_loop(0, 7, drain, 0)
    for k in range(6):
        d2d_copy(k, 7, dp).wait_send()
        d2d_copy(k, 7, dp).wait_recv()


def update(count, gg, gd, weights, m, v):
    G, S = (2, 2, 40, FF), (2, 160, D)
    any_ = pl.BlockSpec(memory_space=pl.ANY)
    dma, vmem = pltpu.SemaphoreType.DMA, pltpu.VMEM
    return pl.pallas_call(
        functools.partial(update_kernel, count),
        out_shape=[
            *(jax.ShapeDtypeStruct(t.shape, BF16) for t in weights),
            *(jax.ShapeDtypeStruct(t.shape, F32) for t in (*m, *v)),
        ],
        in_specs=[pl.BlockSpec(memory_space=pltpu.HBM)] * 11,
        out_specs=[any_] * 9,
        scratch_shapes=[
            vmem(G, BF16), vmem(S, BF16), vmem(G, F32), vmem(S, F32), vmem(G, F32), vmem(S, F32), vmem(G, BF16), vmem(S, BF16),
            vmem((16, 8, 128), F32),
            dma((2,)), dma((6, 3)), dma((16,)), dma((16,)),
            dma((6, 7)), dma((6, 7)), dma((6, 8)), dma((6, 8)), dma((6, 3)),
        ],
        compiler_params=pltpu.CompilerParams(
            collective_id=0, has_side_effects=True, vmem_limit_bytes=16 * 1024 * 1024),
    )(*(pltpu.with_memory_space_constraint(t, pltpu.HBM) for t in (gg, gd, *weights, *m, *v)))


def out_kernel(n, *refs):
    copies = [pltpu.make_async_copy(refs[i], refs[n + i], refs[2 * n].at[i]) for i in range(n)]
    for c in copies:
        c.start()
    for c in copies:
        c.wait()


def put_out(arrays):
    n = len(arrays)
    return pl.pallas_call(
        functools.partial(out_kernel, n),
        out_shape=[jax.ShapeDtypeStruct(t.shape, t.dtype) for t in arrays],
        in_specs=[pl.BlockSpec(memory_space=pl.ANY)] * n,
        out_specs=[pl.BlockSpec(memory_space=pltpu.HBM)] * n,
        scratch_shapes=[pltpu.SemaphoreType.DMA((n,))],
        compiler_params=pltpu.CompilerParams(vmem_limit_bytes=1024 * 1024),
    )(*arrays)


def solution(mesh):
    def body(x, dy, *arrays):
        weights, m, v = (arrays[i : i + 3] for i in (0, 3, 6))
        gg, gd = grads(x[0], dy[0], *weights)
        blocks = [w.reshape(2, 16, -1, w.shape[-1]) for w in weights]
        count = float(sum(w.size for w in weights))
        out = put_out(update(count, gg, gd, blocks, m, v))
        return (*(o.reshape(w.shape) for o, w in zip(out[:3], weights)), *out[3:])

    whole, rows = P(None, None, None), P(None, "dp", None)
    return jax.shard_map(
        body,
        mesh=mesh,
        in_specs=(P(("rep", "dp"), None, None),) * 2 + (whole,) * 3 + (rows,) * 6,
        out_specs=(P("rep", None, None),) * 3 + (P("rep", "dp", None),) * 6,
        check_vma=False,
    )
```

```python
import functools

import jax
import jax.numpy as jnp
from jax import lax
from jax.experimental import pallas as pl
from jax.experimental.pallas import tpu as pltpu
from jax.sharding import PartitionSpec as P

F32, BF16 = jnp.float32, jnp.bfloat16
MESH = pl.DeviceIdType.MESH

T, D, FF = 2048, 640, 2560
F = 256
TILES = FF // F
R = 512
STEPS = T // R
PIECE = 64
DEPTH = 4
UP, DOWN = 4, 3
HOPS = UP + DOWN
ROUNDS = UP + 1
L0 = TILES + 2
LAST = L0 + TILES


def ring(p):
    return p + (p // 4) * (11 - 2 * p)


def dot(a, b):
    return jnp.dot(a, b, preferred_element_type=F32)


def dot_nt(a, b):
    return lax.dot_general(a, b, (((1,), (1,)), ((), ())), preferred_element_type=F32)


def dot_tn(a, b):
    return lax.dot_general(a, b, (((0,), (0,)), ((), ())), preferred_element_type=F32)


def sigmoid(x):
    return jax.nn.sigmoid(x)


def scale_of(wide):
    return lax.rsqrt(jnp.mean(wide * wide, -1, keepdims=True) + 1e-6)


def where_am_i():
    rep, dp = lax.axis_index("rep"), lax.axis_index("dp")
    chip, core = dp // 2, dp % 2
    way = 1 - 2 * core
    return rep, dp, chip, core, way, ring(chip)


def remote(src, dst, send, recv, rep, device):
    return pltpu.make_async_remote_copy(
        src_ref=src, dst_ref=dst, send_sem=send, recv_sem=recv, device_id=(rep, device), device_id_type=MESH)


def grad_kernel(x_hbm, dy_hbm, wg_hbm, wu_hbm, wd_hbm,
                gg_hbm, gd_hbm, gu_hbm, hid_hbm,
                h, a, a0t, a1t, dy, acc, hid, dg, du, wg, wu, wd, wgt, wut, wdt, gu,
                own, other, hop, ownd, otherd, hopd, gg, gd,
                io_sem, w_sem, gu_sem, hid_sem,
                half_send, half_recv, hop_send, hop_recv, dhalf_send, dhalf_recv, dhop_send, dhop_recv):
    rep, dp, chip, core, way, place = where_am_i()
    to = 2 * ring((place + way + 8) % 8) + core
    back = 2 * ring((place - way + 8) % 8) + core
    partner = dp + way

    barrier = pltpu.get_barrier_semaphore()
    for device in (to, back, partner):
        pl.semaphore_signal(barrier, inc=1, device_id=(rep, device), device_id_type=MESH)

    x_copy = pltpu.make_async_copy(x_hbm, h, io_sem.at[0])
    dy_copy = pltpu.make_async_copy(dy_hbm, dy, io_sem.at[1])
    x_copy.start()

    def cols(j):
        return pl.ds(pl.multiple_of(j * F, F), F)

    def rows(t):
        return pl.ds(t * R, R) if isinstance(t, int) else pl.ds(pl.multiple_of(t * R, R), R)

    def w_copies(k):
        layer, j, slot = (k // TILES) % 2, k % TILES, k % 2
        return (
            pltpu.make_async_copy(wg_hbm.at[layer, :, cols(j)], wg.at[slot], w_sem.at[0, slot]),
            pltpu.make_async_copy(wu_hbm.at[layer, :, cols(j)], wu.at[slot], w_sem.at[1, slot]),
            pltpu.make_async_copy(wd_hbm.at[layer, cols(j), :], wd.at[slot], w_sem.at[2, slot]),
        )

    def w_start(k):
        for c in w_copies(k):
            c.start()

    def w_wait(k):
        for c in w_copies(k):
            c.wait()

    def gu_copies(k, out):
        j, t, slot = k // STEPS, k % STEPS, k % DEPTH
        for n in range(2):
            there, here = gu_hbm.at[n, j, rows(t), :], gu.at[slot, n]
            yield pltpu.make_async_copy(here, there, gu_sem.at[n, slot]) if out else pltpu.make_async_copy(
                there, here, gu_sem.at[n, slot])

    def hid_copy(j, out):
        there, here = hid_hbm.at[j], hid.at[j % 3]
        return (pltpu.make_async_copy(here, there, hid_sem.at[j % 3]) if out
                else pltpu.make_async_copy(there, here, hid_sem.at[j % 3]))

    w_start(0)
    x_copy.wait()
    dy_copy.start()

    def ahead(s):
        return (place + way * (UP - s) + 16) % 8

    def behind(s):
        return (place - way * (DOWN - s) + 16) % 8

    def half(i):
        return remote(own.at[i % TILES, :, 1 - core], other.at[i], half_send.at[i], half_recv.at[i], rep, partner)

    def hop_copy(i, slot, src):
        return remote(src, hop.at[i, slot], hop_send.at[i, slot], hop_recv.at[i, slot], rep, to if slot < UP else back)

    def added(i, who):
        return own.at[i % TILES, who, core][...].astype(F32) + other.at[i, who][...].astype(F32)

    def half_d(d, who):
        rows_ = pl.ds(pl.multiple_of((2 * who + 1 - core) * 160, 32), 160)
        return remote(ownd.at[d, rows_], otherd.at[d, who], dhalf_send.at[d, who], dhalf_recv.at[d, who], rep, partner)

    def hop_copy_d(d, slot, src, device):
        return remote(src, hopd.at[d, slot], dhop_send.at[d, slot], dhop_recv.at[d, slot], rep, device)

    def rows_d(who):
        return pl.ds(pl.multiple_of((2 * who + core) * 160, 32), 160)

    def added_d(d, who):
        half_d(d, who).wait_recv()
        return ownd.at[d, rows_d(who)][...].astype(F32) + otherd.at[d, who][...].astype(F32)

    def serve(n):
        for age in range(1, ROUNDS + 1):
            c = n - age
            late = jnp.where(c >= L0, 1, 0)
            i = c - 2 * late

            @pl.when(((c >= 0) & (c < TILES)) | ((c >= L0) & (c < LAST)))
            def _():
                s = age - 1
                if s == 0:
                    half(i).wait_recv()
                    for slot, p in ((0, ahead(0)), (UP, behind(0))):
                        mine = own.at[i % TILES, ring(p), core]
                        mine[...] = added(i, ring(p)).astype(BF16)
                        hop_copy(i, slot, mine).start()
                elif s < UP:
                    for slot, p in ((s, ahead(s)), (UP + s, behind(s)))[: 2 if s < DOWN else 1]:
                        before = hop.at[i, slot - 1]
                        hop_copy(i, slot - 1, before).wait_recv()
                        before[...] = (before[...].astype(F32) + added(i, ring(p))).astype(BF16)
                        hop_copy(i, slot, before).start()
                else:
                    one, two = hop.at[i, UP - 1], hop.at[i, HOPS - 1]
                    hop_copy(i, UP - 1, one).wait_recv()
                    hop_copy(i, HOPS - 1, two).wait_recv()
                    new = (one[...].astype(F32) + two[...].astype(F32) + added(i, chip)).astype(BF16)
                    gg.at[1 - late][:, :, cols(i % TILES)] = new
                    half(i).wait_send()
                    for r in range(HOPS):
                        hop_copy(i, r, one).wait_send()

    def quarter(p):
        t = p // 2
        return t + (t // 2) * (5 - 2 * t)

    def ready(q):
        return (5 * (q + 1) - 1) // 2

    def serve_d(d, q, age):
        s = age - 1
        for base, hops, place_of, device in ((0, UP, ahead, to), (UP, DOWN, behind, back)):
            p = place_of(s)
            here = quarter(p) == q

            @pl.when((s == 0) & here)
            def _():
                mine = ownd.at[d, rows_d(ring(p))]
                mine[...] = added_d(d, ring(p)).astype(BF16)
                hop_copy_d(d, base, mine, device).start()

            @pl.when((s > 0) & (s < hops) & here)
            def _():
                before = hopd.at[d, base + s - 1]
                hop_copy_d(d, base + s - 1, before, device).wait_recv()
                before[...] = (before[...].astype(F32) + added_d(d, ring(p))).astype(BF16)
                hop_copy_d(d, base + s, before, device).start()

        @pl.when((s == UP) & (quarter(place) == q))
        def _():
            one, two = hopd.at[d, UP - 1], hopd.at[d, HOPS - 1]
            hop_copy_d(d, UP - 1, one, to).wait_recv()
            hop_copy_d(d, HOPS - 1, two, back).wait_recv()
            gd.at[d][...] = (one[...].astype(F32) + two[...].astype(F32) + added_d(d, chip)).astype(BF16)

    def put(i, n, t_, grad):
        g = dot(t_[...], grad[...]).astype(BF16)
        for o in range(16):
            own.at[i % TILES, o // 2, o % 2, n][...] = g[40 * o : 40 * o + 40]

    def pieces(t):
        for i in range(0, R, PIECE):
            at = t * R + i
            yield slice(i, i + PIECE), pl.ds(at if isinstance(t, int) else pl.multiple_of(at, PIECE), PIECE)

    def norm(t, to_t):
        wide = h[rows(t), :].astype(F32)
        one = (wide * scale_of(wide)).astype(BF16)
        a[rows(t), :] = one
        to_t[:, rows(t)] = one.T
        acc[rows(t), :] = jnp.zeros((R, D), F32)

    def first(t, z):
        norm(t, a0t)
        return z

    lax.fori_loop(0, STEPS, first, 0)

    hid.at[2][rows(STEPS - 1), :] = jnp.zeros((R, F), BF16)
    wd.at[1][...] = jnp.zeros((F, D), BF16)

    def forward(j, z):
        w_wait(j)

        @pl.when(j >= 3)
        def _():
            hid_copy(j - 3, True).wait()

        def step(t, before):
            k = j * STEPS + t
            h_slot, w_slot, t_before = before
            acc[rows(t_before), :] += dot(hid[h_slot, rows(t_before), :], wd[w_slot])
            gate, up = dot(a[rows(t), :], wg[j % 2]), dot(a[rows(t), :], wu[j % 2])

            @pl.when(k >= DEPTH)
            def _():
                for c in gu_copies(k - DEPTH, True):
                    c.wait()

            for here, there in pieces(t):
                one, two = gate[here], up[here]
                gu.at[k % DEPTH, 0][here, :] = one
                gu.at[k % DEPTH, 1][here, :] = two
                hid.at[j % 3][there, :] = (one * sigmoid(one) * two).astype(BF16)
            for c in gu_copies(k, True):
                c.start()

        step(0, ((j + 2) % 3, (j + 1) % 2, STEPS - 1))
        w_start(j + 1)
        for t in range(1, STEPS):
            step(t, (j % 3, j % 2, t - 1))
        hid_copy(j, True).start()
        return z

    lax.fori_loop(0, TILES, forward, 0)
    acc[rows(STEPS - 1), :] += dot(hid[(TILES - 1) % 3, rows(STEPS - 1), :], wd[(TILES - 1) % 2])
    for k in range(TILES * STEPS - DEPTH, TILES * STEPS):
        for c in gu_copies(k, True):
            c.wait()
    for j in range(TILES - 3, TILES):
        hid_copy(j, True).wait()

    def second(t, z):
        h[rows(t), :] = (h[rows(t), :].astype(F32) + acc[rows(t), :].astype(BF16).astype(F32)).astype(BF16)
        norm(t, a1t)
        return z

    lax.fori_loop(0, STEPS, second, 0)
    dy_copy.wait()
    pl.semaphore_wait(barrier, 3)

    def back_of(gate, up, by_hidden, there, to_hidden=None):
        sig = sigmoid(gate)
        silu = gate * sig
        dg[there, :] = (by_hidden * up * (sig + silu * (1.0 - sig))).astype(BF16)
        du[there, :] = (by_hidden * silu).astype(BF16)
        if to_hidden is not None:
            to_hidden[there, :] = (silu * up).astype(BF16)

    def tile(j, z):
        k = TILES + j
        slot = k % 2
        w_wait(k)
        w_start(k + 1)

        def step(t, z):
            gate, up = dot(a[rows(t), :], wg[slot]), dot(a[rows(t), :], wu[slot])
            by_hidden = dot(dy[rows(t), :], wdt[...]).astype(BF16).astype(F32)
            for here, there in pieces(t):
                back_of(gate[here], up[here], by_hidden[here], there, hid.at[0])
            return z

        wdt[...] = wd[slot].T
        for t in range(STEPS):
            step(t, 0)
        serve(j)

        def quarters(q, z):
            serve_d(1, q, j - ready(q))
            return z

        lax.fori_loop(0, 3, quarters, 0)
        wgt[...] = wg[slot].T
        wut[...] = wu[slot].T
        put(j, 0, a1t, dg)
        put(j, 1, a1t, du)
        half(j).start()
        ownd.at[1][cols(j), :] = dot_tn(hid[0], dy[...]).astype(BF16)

        for q in range(4):
            @pl.when(j == ready(q))
            def _():
                half_d(1, 2 * q).start()
                half_d(1, 2 * q + 1).start()


        def step_a(t, z):
            acc[rows(t), :] += dot(dg[rows(t), :], wgt[...]) + dot(du[rows(t), :], wut[...])
            return z

        @pl.when(j == 0)
        def _():
            def clear(t, z):
                acc[rows(t), :] = jnp.zeros((R, D), F32)
                return z
            lax.fori_loop(0, STEPS, clear, 0)

        lax.fori_loop(0, STEPS, step_a, 0)
        return z

    lax.fori_loop(0, TILES, tile, 0)
    hid_copy(0, False).start()
    hid_copy(1, False).start()
    for k in range(DEPTH - 1):
        for c in gu_copies(k, False):
            c.start()

    def by_h(t, z):
        by_a = acc[rows(t), :].astype(BF16).astype(F32)
        wide = h[rows(t), :].astype(F32)
        scale = scale_of(wide)
        by_wide = scale * by_a - wide * (scale * scale * scale * jnp.mean(by_a * wide, -1, keepdims=True))
        dy[rows(t), :] = (dy[rows(t), :].astype(F32) + by_wide.astype(BF16).astype(F32)).astype(BF16)
        return z

    lax.fori_loop(0, STEPS, by_h, 0)

    def down(r, z):
        def one(jj, z):
            j = r * (TILES // 2) + jj
            hid_copy(j, False).wait()

            @pl.when(j + 2 < TILES)
            def _():
                hid_copy(j + 2, False).start()

            ownd.at[0][cols(j), :] = dot_tn(hid[j % 3], dy[...]).astype(BF16)
            return z

        lax.fori_loop(0, TILES // 2, one, 0)
        for i in range(4):
            half_d(0, 4 * r + i).start()
        serve(TILES + r)

        def quarters(q, z):
            serve_d(1, q, TILES + r - ready(q))
            return z

        lax.fori_loop(0, 4, quarters, 0)
        return z

    lax.fori_loop(0, 2, down, 0)

    def wd_copy(k):
        return pltpu.make_async_copy(wd_hbm.at[0, cols(k % TILES), :], wd.at[k % 2], w_sem.at[2, k % 2])

    w_wait(2 * TILES)
    wd_copy(2 * TILES + 1).start()

    def by_hidden(t, z):
        hid.at[0][rows(t), :] = dot_nt(dy[rows(t), :], wd[0]).astype(BF16)
        return z

    lax.fori_loop(0, STEPS, by_hidden, 0)

    def tile0(j, z):
        k = 2 * TILES + j

        @pl.when(j + 1 < TILES)
        def _():
            wd_copy(k + 1).wait()

        @pl.when(j + 2 < TILES)
        def _():
            wd_copy(k + 2).start()

        def step(t, z):
            n = j * STEPS + t
            for c in gu_copies(n, False):
                c.wait()

            @pl.when(n + DEPTH - 1 < TILES * STEPS)
            def _():
                for c in gu_copies(n + DEPTH - 1, False):
                    c.start()

            hid.at[(j + 1) % 2][rows(t), :] = dot_nt(dy[rows(t), :], wd[(j + 1) % 2]).astype(BF16)
            for here, there in pieces(t):
                back_of(gu[n % DEPTH, 0, here, :], gu[n % DEPTH, 1, here, :], hid[j % 2, there, :].astype(F32), there)
            return z

        lax.fori_loop(0, STEPS, step, 0)
        serve(L0 + j)

        def quarters(q, z):
            serve_d(1, q, L0 + j - ready(q))
            serve_d(0, q, jnp.where(j % 2 == 0, j // 2 + 1, 0))
            return z

        lax.fori_loop(0, 4, quarters, 0)
        put(TILES + j, 0, a0t, dg)
        put(TILES + j, 1, a0t, du)
        half(TILES + j).start()
        return z

    lax.fori_loop(0, TILES, tile0, 0)

    def drain(r, z):
        serve(LAST + r)
        return z

    lax.fori_loop(0, ROUNDS, drain, 0)
    for d in range(2):
        for who in range(8):
            half_d(d, who).wait_send()
        for slot in range(HOPS):
            hop_copy_d(d, slot, hopd.at[d, slot], to).wait_send()
    out = [pltpu.make_async_copy(gg, gg_hbm, io_sem.at[0]), pltpu.make_async_copy(gd, gd_hbm, io_sem.at[1])]
    for c in out:
        c.start()
    for c in out:
        c.wait()


def grads(x, dy, wg, wu, wd):
    any_ = pl.BlockSpec(memory_space=pl.ANY)
    dma, vmem = pltpu.SemaphoreType.DMA, pltpu.VMEM
    s = jax.ShapeDtypeStruct
    block = (2, 40, F)
    out = pl.pallas_call(
        grad_kernel,
        out_shape=[s((2, 2, 40, FF), BF16), s((2, 160, D), BF16),
                   s((2, TILES, T, F), F32), s((TILES, T, F), BF16)],
        in_specs=[any_] * 5,
        out_specs=[any_] * 4,
        scratch_shapes=[
            vmem((T, D), BF16), vmem((T, D), BF16), vmem((D, T), BF16), vmem((D, T), BF16), vmem((T, D), BF16),
            vmem((T, D), F32), vmem((3, T, F), BF16), vmem((T, F), BF16), vmem((T, F), BF16),
            vmem((2, D, F), BF16), vmem((2, D, F), BF16), vmem((2, F, D), BF16),
            vmem((F, D), BF16), vmem((F, D), BF16), vmem((D, F), BF16), vmem((DEPTH, 2, R, F), F32),
            vmem((TILES, 8, 2, *block), BF16), vmem((2 * TILES, 8, *block), BF16), vmem((2 * TILES, HOPS, *block), BF16),
            vmem((2, FF, D), BF16), vmem((2, 8, 160, D), BF16), vmem((2, HOPS, 160, D), BF16),
            vmem((2, 2, 40, FF), BF16), vmem((2, 160, D), BF16),
            dma((2,)), dma((3, 2)), dma((2, DEPTH)), dma((3,)),
            dma((2 * TILES,)), dma((2 * TILES,)), dma((2 * TILES, HOPS)), dma((2 * TILES, HOPS)),
            dma((2, 8)), dma((2, 8)), dma((2, HOPS)), dma((2, HOPS)),
        ],
        compiler_params=pltpu.CompilerParams(
            collective_id=1, has_side_effects=True, vmem_limit_bytes=67043328),
    )(x, dy, wg, wu, wd)
    return out[:2]


def update_kernel(count, *refs):
    gg_hbm, gd_hbm, w, m, v = refs[0], refs[1], refs[2:5], refs[5:8], refs[8:11]
    w_out, m_out, v_out = refs[11:14], refs[14:17], refs[17:20]
    (gg, gd, mg, md, vg, vd, wg, wd, sums, g_sem, load_sem, sum_send, sum_recv,
     ag_send, ag_recv, d2d_send, d2d_recv, store_sem) = refs[20:]
    items = [(0, 0), (1, 0), (2, 0), (0, 1), (1, 1), (2, 1)]

    def at(k, big, small):
        which, layer_ = items[k]
        return small.at[layer_] if which == 2 else big.at[layer_, which]

    rep, dp, chip, core, way, place = where_am_i()
    to = 2 * ring((place + way + 8) % 8) + core
    partner = dp + way

    barrier = pltpu.get_barrier_semaphore()
    for off in range(1, 16):
        pl.semaphore_signal(barrier, inc=1, device_id=(rep, (dp + off) % 16), device_id_type=MESH)

    g_loads = [pltpu.make_async_copy(gg_hbm, gg, g_sem.at[0]), pltpu.make_async_copy(gd_hbm, gd, g_sem.at[1])]
    for c in g_loads:
        c.start()
    loads = []
    for k, (which, layer_) in enumerate(items):
        for n, (src, dst) in enumerate((
            (m[which].at[layer_], at(k, mg, md)),
            (v[which].at[layer_], at(k, vg, vd)),
            (w[which].at[layer_, dp], at(k, wg, wd)),
        )):
            c = pltpu.make_async_copy(src, dst, load_sem.at[k, n])
            c.start()
            loads.append(c)
    for c in g_loads:
        c.wait()

    squares = jnp.zeros((8, 128), F32)
    for k in range(6):
        g = at(k, gg, gd)[...].astype(F32)
        g = g * g
        part = g[0:8]
        for i in range(1, g.shape[0] // 8):
            part = part + g[8 * i : 8 * i + 8]
        for i in range(part.shape[1] // 128):
            squares = squares + part[:, 128 * i : 128 * i + 128]
    sums.at[dp][...] = squares
    pl.semaphore_wait(barrier, 15)

    def sum_copy(off):
        return remote(sums.at[dp], sums.at[dp], sum_send.at[off], sum_recv.at[off], rep, (dp + off) % 16)

    for off in range(1, 16):
        sum_copy(off).start()
    for c in loads:
        c.wait()
    for off in range(1, 16):
        sum_copy(off).wait_recv()
    mean = jnp.sum(sums[...]) / count
    factor = jnp.minimum(1.0, 0.5 * lax.rsqrt(jnp.full((8, 128), mean + 1e-30, F32)))[0:1, 0:1]

    def block(k, who):
        which, layer_ = items[k]
        return w_out[which].at[layer_, who]

    def gather_copy(k, s, who, src=None):
        src = block(k, who) if src is None else src
        return remote(src, block(k, who), ag_send.at[k, s], ag_recv.at[k, s], rep, to)

    def d2d_copy(k, s, who, src=None):
        src = block(k, who) if src is None else src
        return remote(src, block(k, who), d2d_send.at[k, s], d2d_recv.at[k, s], rep, partner)

    stores = []
    for k, (which, layer_) in enumerate(items):
        g = at(k, gg, gd)[...].astype(F32) * factor
        mk, vk, wk = at(k, mg, md), at(k, vg, vd), at(k, wg, wd)
        new_m = 0.9 * mk[...] + 0.1 * g
        new_v = 0.95 * vk[...] + 0.05 * g * g
        wide = wk[...].astype(F32)
        wk[...] = (wide - 0.02 * (new_m * lax.rsqrt(new_v + 1e-8) + 0.1 * wide)).astype(BF16)
        mk[...] = new_m
        vk[...] = new_v
        gather_copy(k, 0, dp, wk).start()
        d2d_copy(k, 0, dp, wk).start()
        for n, (src, dst) in enumerate((
            (wk, block(k, dp)), (mk, m_out[which].at[layer_]), (vk, v_out[which].at[layer_]))):
            c = pltpu.make_async_copy(src, dst, store_sem.at[k, n])
            c.start()
            stores.append(c)

    def source(s):
        return 2 * ring((place - way * (1 + s) + 16) % 8) + core

    def gather(s, z):
        for k in range(6):
            who = source(s)
            gather_copy(k, s, who).wait_recv()
            gather_copy(k, s + 1, who).start()
            d2d_copy(k, s + 1, who).start()
        return z

    lax.fori_loop(0, 6, gather, 0)
    for k in range(6):
        who = source(6)
        gather_copy(k, 6, who).wait_recv()
        d2d_copy(k, 7, who).start()

    for c in stores:
        c.wait()
    for off in range(1, 16):
        sum_copy(off).wait_send()

    def drain(s, z):
        for k in range(6):
            gather_copy(k, s, dp).wait_send()
            d2d_copy(k, s, dp).wait_send()
            d2d_copy(k, s, dp).wait_recv()
        return z

    lax.fori_loop(0, 7, drain, 0)
    for k in range(6):
        d2d_copy(k, 7, dp).wait_send()
        d2d_copy(k, 7, dp).wait_recv()


def update(count, gg, gd, weights, m, v):
    G, S = (2, 2, 40, FF), (2, 160, D)
    any_ = pl.BlockSpec(memory_space=pl.ANY)
    dma, vmem = pltpu.SemaphoreType.DMA, pltpu.VMEM
    return pl.pallas_call(
        functools.partial(update_kernel, count),
        out_shape=[
            *(jax.ShapeDtypeStruct(t.shape, BF16) for t in weights),
            *(jax.ShapeDtypeStruct(t.shape, F32) for t in (*m, *v)),
        ],
        in_specs=[pl.BlockSpec(memory_space=pltpu.HBM)] * 11,
        out_specs=[any_] * 9,
        scratch_shapes=[
            vmem(G, BF16), vmem(S, BF16), vmem(G, F32), vmem(S, F32), vmem(G, F32), vmem(S, F32), vmem(G, BF16), vmem(S, BF16),
            vmem((16, 8, 128), F32),
            dma((2,)), dma((6, 3)), dma((16,)), dma((16,)),
            dma((6, 7)), dma((6, 7)), dma((6, 8)), dma((6, 8)), dma((6, 3)),
        ],
        compiler_params=pltpu.CompilerParams(
            collective_id=0, has_side_effects=True, vmem_limit_bytes=16 * 1024 * 1024),
    )(*(pltpu.with_memory_space_constraint(t, pltpu.HBM) for t in (gg, gd, *weights, *m, *v)))


def out_kernel(n, *refs):
    copies = [pltpu.make_async_copy(refs[i], refs[n + i], refs[2 * n].at[i]) for i in range(n)]
    for c in copies:
        c.start()
    for c in copies:
        c.wait()


def put_out(arrays):
    n = len(arrays)
    return pl.pallas_call(
        functools.partial(out_kernel, n),
        out_shape=[jax.ShapeDtypeStruct(t.shape, t.dtype) for t in arrays],
        in_specs=[pl.BlockSpec(memory_space=pl.ANY)] * n,
        out_specs=[pl.BlockSpec(memory_space=pltpu.HBM)] * n,
        scratch_shapes=[pltpu.SemaphoreType.DMA((n,))],
        compiler_params=pltpu.CompilerParams(vmem_limit_bytes=1024 * 1024),
    )(*arrays)


def solution(mesh):
    def body(x, dy, *arrays):
        weights, m, v = (arrays[i : i + 3] for i in (0, 3, 6))
        gg, gd = grads(x[0], dy[0], *weights)
        blocks = [w.reshape(2, 16, -1, w.shape[-1]) for w in weights]
        count = float(sum(w.size for w in weights))
        out = put_out(update(count, gg, gd, blocks, m, v))
        return (*(o.reshape(w.shape) for o, w in zip(out[:3], weights)), *out[3:])

    whole, rows = P(None, None, None), P(None, "dp", None)
    return jax.shard_map(
        body,
        mesh=mesh,
        in_specs=(P(("rep", "dp"), None, None),) * 2 + (whole,) * 3 + (rows,) * 6,
        out_specs=(P("rep", None, None),) * 3 + (P("rep", "dp", None),) * 6,
        check_vma=False,
    )
```

```python
import functools

import jax
import jax.numpy as jnp
from jax import lax
from jax.experimental import pallas as pl
from jax.experimental.pallas import tpu as pltpu
from jax.sharding import PartitionSpec as P

F32, BF16 = jnp.float32, jnp.bfloat16
MESH = pl.DeviceIdType.MESH

T, D, FF = 2048, 640, 2560
F = 256
TILES = FF // F
R = 512
STEPS = T // R
PIECE = 64
DEPTH = 4
UP, DOWN = 4, 3
HOPS = UP + DOWN
ROUNDS = UP + 1
L0 = TILES + 2
LAST = L0 + TILES


def ring(p):
    return p + (p // 4) * (11 - 2 * p)


def dot(a, b):
    return jnp.dot(a, b, preferred_element_type=F32)


def dot_nt(a, b):
    return lax.dot_general(a, b, (((1,), (1,)), ((), ())), preferred_element_type=F32)


def dot_tn(a, b):
    return lax.dot_general(a, b, (((0,), (0,)), ((), ())), preferred_element_type=F32)


def sigmoid(x):
    return jax.nn.sigmoid(x)


def scale_of(wide):
    return lax.rsqrt(jnp.mean(wide * wide, -1, keepdims=True) + 1e-6)


def where_am_i():
    rep, dp = lax.axis_index("rep"), lax.axis_index("dp")
    chip, core = dp // 2, dp % 2
    way = 1 - 2 * core
    return rep, dp, chip, core, way, ring(chip)


def remote(src, dst, send, recv, rep, device):
    return pltpu.make_async_remote_copy(
        src_ref=src, dst_ref=dst, send_sem=send, recv_sem=recv, device_id=(rep, device), device_id_type=MESH)


def grad_kernel(x_hbm, dy_hbm, wg_hbm, wu_hbm, wd_hbm,
                gg_hbm, gd_hbm, gu_hbm, hid_hbm,
                h, a, a0t, a1t, dy, acc, hid, dg, du, wg, wu, wd, wgt, wut, wdt, gu,
                own, other, hop, ownd, otherd, hopd, gg, gd,
                io_sem, w_sem, gu_sem, hid_sem,
                half_send, half_recv, hop_send, hop_recv, dhalf_send, dhalf_recv, dhop_send, dhop_recv):
    rep, dp, chip, core, way, place = where_am_i()
    to = 2 * ring((place + way + 8) % 8) + core
    back = 2 * ring((place - way + 8) % 8) + core
    partner = dp + way

    barrier = pltpu.get_barrier_semaphore()
    for device in (to, back, partner):
        pl.semaphore_signal(barrier, inc=1, device_id=(rep, device), device_id_type=MESH)

    x_copy = pltpu.make_async_copy(x_hbm, h, io_sem.at[0])
    dy_copy = pltpu.make_async_copy(dy_hbm, dy, io_sem.at[1])
    x_copy.start()

    def cols(j):
        return pl.ds(pl.multiple_of(j * F, F), F)

    def rows(t):
        return pl.ds(t * R, R) if isinstance(t, int) else pl.ds(pl.multiple_of(t * R, R), R)

    def w_copies(k):
        layer, j, slot = (k // TILES) % 2, k % TILES, k % 2
        return (
            pltpu.make_async_copy(wg_hbm.at[layer, :, cols(j)], wg.at[slot], w_sem.at[0, slot]),
            pltpu.make_async_copy(wu_hbm.at[layer, :, cols(j)], wu.at[slot], w_sem.at[1, slot]),
            pltpu.make_async_copy(wd_hbm.at[layer, cols(j), :], wd.at[slot], w_sem.at[2, slot]),
        )

    def w_start(k):
        for c in w_copies(k):
            c.start()

    def w_wait(k):
        for c in w_copies(k):
            c.wait()

    def gu_copies(k, out):
        j, t, slot = k // STEPS, k % STEPS, k % DEPTH
        for n in range(2):
            there, here = gu_hbm.at[n, j, rows(t), :], gu.at[slot, n]
            yield pltpu.make_async_copy(here, there, gu_sem.at[n, slot]) if out else pltpu.make_async_copy(
                there, here, gu_sem.at[n, slot])

    def hid_copy(j, out):
        there, here = hid_hbm.at[j], hid.at[j % 3]
        return (pltpu.make_async_copy(here, there, hid_sem.at[j % 3]) if out
                else pltpu.make_async_copy(there, here, hid_sem.at[j % 3]))

    w_start(0)
    x_copy.wait()
    dy_copy.start()

    def ahead(s):
        return (place + way * (UP - s) + 16) % 8

    def behind(s):
        return (place - way * (DOWN - s) + 16) % 8

    def half(i):
        return remote(own.at[i % TILES, :, 1 - core], other.at[i], half_send.at[i], half_recv.at[i], rep, partner)

    def hop_copy(i, slot, src):
        return remote(src, hop.at[i, slot], hop_send.at[i, slot], hop_recv.at[i, slot], rep, to if slot < UP else back)

    def added(i, who):
        return own.at[i % TILES, who, core][...].astype(F32) + other.at[i, who][...].astype(F32)

    def half_d(d, who):
        rows_ = pl.ds(pl.multiple_of((2 * who + 1 - core) * 160, 32), 160)
        return remote(ownd.at[d, rows_], otherd.at[d, who], dhalf_send.at[d, who], dhalf_recv.at[d, who], rep, partner)

    def hop_copy_d(d, slot, src, device):
        return remote(src, hopd.at[d, slot], dhop_send.at[d, slot], dhop_recv.at[d, slot], rep, device)

    def rows_d(who):
        return pl.ds(pl.multiple_of((2 * who + core) * 160, 32), 160)

    def added_d(d, who):
        half_d(d, who).wait_recv()
        return ownd.at[d, rows_d(who)][...].astype(F32) + otherd.at[d, who][...].astype(F32)

    def serve(n):
        for age in range(1, ROUNDS + 1):
            c = n - age
            late = jnp.where(c >= L0, 1, 0)
            i = c - 2 * late

            @pl.when(((c >= 0) & (c < TILES)) | ((c >= L0) & (c < LAST)))
            def _():
                s = age - 1
                if s == 0:
                    half(i).wait_recv()
                    for slot, p in ((0, ahead(0)), (UP, behind(0))):
                        mine = own.at[i % TILES, ring(p), core]
                        mine[...] = added(i, ring(p)).astype(BF16)
                        hop_copy(i, slot, mine).start()
                elif s < UP:
                    for slot, p in ((s, ahead(s)), (UP + s, behind(s)))[: 2 if s < DOWN else 1]:
                        before = hop.at[i, slot - 1]
                        hop_copy(i, slot - 1, before).wait_recv()
                        before[...] = (before[...].astype(F32) + added(i, ring(p))).astype(BF16)
                        hop_copy(i, slot, before).start()
                else:
                    one, two = hop.at[i, UP - 1], hop.at[i, HOPS - 1]
                    hop_copy(i, UP - 1, one).wait_recv()
                    hop_copy(i, HOPS - 1, two).wait_recv()
                    new = (one[...].astype(F32) + two[...].astype(F32) + added(i, chip)).astype(BF16)
                    gg.at[1 - late][:, :, cols(i % TILES)] = new
                    half(i).wait_send()
                    for r in range(HOPS):
                        hop_copy(i, r, one).wait_send()

    def quarter(p):
        t = p // 2
        return t + (t // 2) * (5 - 2 * t)

    def ready(q):
        return (5 * (q + 1) - 1) // 2

    def serve_d(d, q, age):
        s = age - 1
        for base, hops, place_of, device in ((0, UP, ahead, to), (UP, DOWN, behind, back)):
            p = place_of(s)
            here = quarter(p) == q

            @pl.when((s == 0) & here)
            def _():
                mine = ownd.at[d, rows_d(ring(p))]
                mine[...] = added_d(d, ring(p)).astype(BF16)
                hop_copy_d(d, base, mine, device).start()

            @pl.when((s > 0) & (s < hops) & here)
            def _():
                before = hopd.at[d, base + s - 1]
                hop_copy_d(d, base + s - 1, before, device).wait_recv()
                before[...] = (before[...].astype(F32) + added_d(d, ring(p))).astype(BF16)
                hop_copy_d(d, base + s, before, device).start()

        @pl.when((s == UP) & (quarter(place) == q))
        def _():
            one, two = hopd.at[d, UP - 1], hopd.at[d, HOPS - 1]
            hop_copy_d(d, UP - 1, one, to).wait_recv()
            hop_copy_d(d, HOPS - 1, two, back).wait_recv()
            gd.at[d][...] = (one[...].astype(F32) + two[...].astype(F32) + added_d(d, chip)).astype(BF16)

    def put(i, n, t_, grad):
        g = dot(t_[...], grad[...]).astype(BF16)
        for o in range(16):
            own.at[i % TILES, o // 2, o % 2, n][...] = g[40 * o : 40 * o + 40]

    def pieces(t):
        for i in range(0, R, PIECE):
            at = t * R + i
            yield slice(i, i + PIECE), pl.ds(at if isinstance(t, int) else pl.multiple_of(at, PIECE), PIECE)

    def norm(t, to_t):
        wide = h[rows(t), :].astype(F32)
        one = (wide * scale_of(wide)).astype(BF16)
        a[rows(t), :] = one
        to_t[:, rows(t)] = one.T
        acc[rows(t), :] = jnp.zeros((R, D), F32)

    def first(t, z):
        norm(t, a0t)
        return z

    lax.fori_loop(0, STEPS, first, 0)

    hid.at[2][rows(STEPS - 1), :] = jnp.zeros((R, F), BF16)
    wd.at[1][...] = jnp.zeros((F, D), BF16)

    def forward(j, z):
        w_wait(j)

        @pl.when(j >= 3)
        def _():
            hid_copy(j - 3, True).wait()

        def step(t, before):
            k = j * STEPS + t
            h_slot, w_slot, t_before = before
            acc[rows(t_before), :] += dot(hid[h_slot, rows(t_before), :], wd[w_slot])
            gate, up = dot(a[rows(t), :], wg[j % 2]), dot(a[rows(t), :], wu[j % 2])

            @pl.when(k >= DEPTH)
            def _():
                for c in gu_copies(k - DEPTH, True):
                    c.wait()

            for here, there in pieces(t):
                one, two = gate[here], up[here]
                gu.at[k % DEPTH, 0][here, :] = one
                gu.at[k % DEPTH, 1][here, :] = two
                hid.at[j % 3][there, :] = (one * sigmoid(one) * two).astype(BF16)
            for c in gu_copies(k, True):
                c.start()

        step(0, ((j + 2) % 3, (j + 1) % 2, STEPS - 1))
        w_start(j + 1)
        for t in range(1, STEPS):
            step(t, (j % 3, j % 2, t - 1))
        hid_copy(j, True).start()
        return z

    lax.fori_loop(0, TILES, forward, 0)
    acc[rows(STEPS - 1), :] += dot(hid[(TILES - 1) % 3, rows(STEPS - 1), :], wd[(TILES - 1) % 2])
    for k in range(TILES * STEPS - DEPTH, TILES * STEPS):
        for c in gu_copies(k, True):
            c.wait()
    for j in range(TILES - 3, TILES):
        hid_copy(j, True).wait()

    def second(t, z):
        h[rows(t), :] = (h[rows(t), :].astype(F32) + acc[rows(t), :].astype(BF16).astype(F32)).astype(BF16)
        norm(t, a1t)
        return z

    lax.fori_loop(0, STEPS, second, 0)
    dy_copy.wait()
    pl.semaphore_wait(barrier, 3)

    def back_of(gate, up, by_hidden, there, to_hidden=None):
        sig = sigmoid(gate)
        silu = gate * sig
        dg[there, :] = (by_hidden * up * (sig + silu * (1.0 - sig))).astype(BF16)
        du[there, :] = (by_hidden * silu).astype(BF16)
        if to_hidden is not None:
            to_hidden[there, :] = (silu * up).astype(BF16)

    def tile(j, z):
        k = TILES + j
        slot = k % 2
        w_wait(k)
        w_start(k + 1)

        def step(t, z):
            gate, up = dot(a[rows(t), :], wg[slot]), dot(a[rows(t), :], wu[slot])
            by_hidden = dot(dy[rows(t), :], wdt[...]).astype(BF16).astype(F32)
            for here, there in pieces(t):
                back_of(gate[here], up[here], by_hidden[here], there, hid.at[0])
            return z

        wdt[...] = wd[slot].T
        for t in range(STEPS):
            step(t, 0)
        serve(j)

        def quarters(q, z):
            serve_d(1, q, j - ready(q))
            return z

        lax.fori_loop(0, 3, quarters, 0)
        wgt[...] = wg[slot].T
        wut[...] = wu[slot].T
        put(j, 0, a1t, dg)
        put(j, 1, a1t, du)
        half(j).start()
        ownd.at[1][cols(j), :] = dot_tn(hid[0], dy[...]).astype(BF16)

        for q in range(4):
            @pl.when(j == ready(q))
            def _():
                half_d(1, 2 * q).start()
                half_d(1, 2 * q + 1).start()


        def step_a(t, z):
            acc[rows(t), :] += dot(dg[rows(t), :], wgt[...]) + dot(du[rows(t), :], wut[...])
            return z

        @pl.when(j == 0)
        def _():
            def clear(t, z):
                acc[rows(t), :] = jnp.zeros((R, D), F32)
                return z
            lax.fori_loop(0, STEPS, clear, 0)

        lax.fori_loop(0, STEPS, step_a, 0)
        return z

    lax.fori_loop(0, TILES, tile, 0)
    hid_copy(0, False).start()
    hid_copy(1, False).start()
    for k in range(DEPTH - 1):
        for c in gu_copies(k, False):
            c.start()

    def by_h(t, z):
        by_a = acc[rows(t), :].astype(BF16).astype(F32)
        wide = h[rows(t), :].astype(F32)
        scale = scale_of(wide)
        by_wide = scale * by_a - wide * (scale * scale * scale * jnp.mean(by_a * wide, -1, keepdims=True))
        dy[rows(t), :] = (dy[rows(t), :].astype(F32) + by_wide.astype(BF16).astype(F32)).astype(BF16)
        return z

    lax.fori_loop(0, STEPS, by_h, 0)

    def down(r, z):
        def one(jj, z):
            j = r * (TILES // 2) + jj
            hid_copy(j, False).wait()

            @pl.when(j + 2 < TILES)
            def _():
                hid_copy(j + 2, False).start()

            ownd.at[0][cols(j), :] = dot_tn(hid[j % 3], dy[...]).astype(BF16)
            return z

        lax.fori_loop(0, TILES // 2, one, 0)
        for i in range(4):
            half_d(0, 4 * r + i).start()
        serve(TILES + r)

        def quarters(q, z):
            serve_d(1, q, TILES + r - ready(q))
            return z

        lax.fori_loop(0, 4, quarters, 0)
        return z

    lax.fori_loop(0, 2, down, 0)

    def wd_copy(k):
        return pltpu.make_async_copy(wd_hbm.at[0, cols(k % TILES), :], wd.at[k % 2], w_sem.at[2, k % 2])

    w_wait(2 * TILES)
    wd_copy(2 * TILES + 1).start()

    def by_hidden(t, z):
        hid.at[0][rows(t), :] = dot_nt(dy[rows(t), :], wd[0]).astype(BF16)
        return z

    lax.fori_loop(0, STEPS, by_hidden, 0)

    def tile0(j, z):
        k = 2 * TILES + j

        @pl.when(j + 1 < TILES)
        def _():
            wd_copy(k + 1).wait()

        @pl.when(j + 2 < TILES)
        def _():
            wd_copy(k + 2).start()

        def step(t, z):
            n = j * STEPS + t
            for c in gu_copies(n, False):
                c.wait()

            @pl.when(n + DEPTH - 1 < TILES * STEPS)
            def _():
                for c in gu_copies(n + DEPTH - 1, False):
                    c.start()

            hid.at[(j + 1) % 2][rows(t), :] = dot_nt(dy[rows(t), :], wd[(j + 1) % 2]).astype(BF16)
            for here, there in pieces(t):
                back_of(gu[n % DEPTH, 0, here, :], gu[n % DEPTH, 1, here, :], hid[j % 2, there, :].astype(F32), there)
            return z

        lax.fori_loop(0, STEPS, step, 0)
        serve(L0 + j)

        @pl.when(j < 3)
        def _():
            for q in (2, 3):
                serve_d(1, q, L0 + j - ready(q))

        @pl.when(j % 2 == 0)
        def _():
            def quarters(q, z):
                serve_d(0, q, j // 2 + 1)
                return z

            lax.fori_loop(0, 4, quarters, 0)

        put(TILES + j, 0, a0t, dg)
        put(TILES + j, 1, a0t, du)
        half(TILES + j).start()
        return z

    lax.fori_loop(0, TILES, tile0, 0)

    def drain(r, z):
        serve(LAST + r)
        return z

    lax.fori_loop(0, ROUNDS, drain, 0)
    for d in range(2):
        for who in range(8):
            half_d(d, who).wait_send()
        for slot in range(HOPS):
            hop_copy_d(d, slot, hopd.at[d, slot], to).wait_send()
    out = [pltpu.make_async_copy(gg, gg_hbm, io_sem.at[0]), pltpu.make_async_copy(gd, gd_hbm, io_sem.at[1])]
    for c in out:
        c.start()
    for c in out:
        c.wait()


def grads(x, dy, wg, wu, wd):
    any_ = pl.BlockSpec(memory_space=pl.ANY)
    dma, vmem = pltpu.SemaphoreType.DMA, pltpu.VMEM
    s = jax.ShapeDtypeStruct
    block = (2, 40, F)
    out = pl.pallas_call(
        grad_kernel,
        out_shape=[s((2, 2, 40, FF), BF16), s((2, 160, D), BF16),
                   s((2, TILES, T, F), F32), s((TILES, T, F), BF16)],
        in_specs=[any_] * 5,
        out_specs=[any_] * 4,
        scratch_shapes=[
            vmem((T, D), BF16), vmem((T, D), BF16), vmem((D, T), BF16), vmem((D, T), BF16), vmem((T, D), BF16),
            vmem((T, D), F32), vmem((3, T, F), BF16), vmem((T, F), BF16), vmem((T, F), BF16),
            vmem((2, D, F), BF16), vmem((2, D, F), BF16), vmem((2, F, D), BF16),
            vmem((F, D), BF16), vmem((F, D), BF16), vmem((D, F), BF16), vmem((DEPTH, 2, R, F), F32),
            vmem((TILES, 8, 2, *block), BF16), vmem((2 * TILES, 8, *block), BF16), vmem((2 * TILES, HOPS, *block), BF16),
            vmem((2, FF, D), BF16), vmem((2, 8, 160, D), BF16), vmem((2, HOPS, 160, D), BF16),
            vmem((2, 2, 40, FF), BF16), vmem((2, 160, D), BF16),
            dma((2,)), dma((3, 2)), dma((2, DEPTH)), dma((3,)),
            dma((2 * TILES,)), dma((2 * TILES,)), dma((2 * TILES, HOPS)), dma((2 * TILES, HOPS)),
            dma((2, 8)), dma((2, 8)), dma((2, HOPS)), dma((2, HOPS)),
        ],
        compiler_params=pltpu.CompilerParams(
            collective_id=1, has_side_effects=True, vmem_limit_bytes=67043328),
    )(x, dy, wg, wu, wd)
    return out[:2]


def update_kernel(count, *refs):
    gg_hbm, gd_hbm, w, m, v = refs[0], refs[1], refs[2:5], refs[5:8], refs[8:11]
    w_out, m_out, v_out = refs[11:14], refs[14:17], refs[17:20]
    (gg, gd, mg, md, vg, vd, wg, wd, sums, g_sem, load_sem, sum_send, sum_recv,
     ag_send, ag_recv, d2d_send, d2d_recv, store_sem) = refs[20:]
    items = [(0, 0), (1, 0), (2, 0), (0, 1), (1, 1), (2, 1)]

    def at(k, big, small):
        which, layer_ = items[k]
        return small.at[layer_] if which == 2 else big.at[layer_, which]

    rep, dp, chip, core, way, place = where_am_i()
    to = 2 * ring((place + way + 8) % 8) + core
    partner = dp + way

    barrier = pltpu.get_barrier_semaphore()
    for off in range(1, 16):
        pl.semaphore_signal(barrier, inc=1, device_id=(rep, (dp + off) % 16), device_id_type=MESH)

    g_loads = [pltpu.make_async_copy(gg_hbm, gg, g_sem.at[0]), pltpu.make_async_copy(gd_hbm, gd, g_sem.at[1])]
    for c in g_loads:
        c.start()
    loads = []
    for k, (which, layer_) in enumerate(items):
        for n, (src, dst) in enumerate((
            (m[which].at[layer_], at(k, mg, md)),
            (v[which].at[layer_], at(k, vg, vd)),
            (w[which].at[layer_, dp], at(k, wg, wd)),
        )):
            c = pltpu.make_async_copy(src, dst, load_sem.at[k, n])
            c.start()
            loads.append(c)
    for c in g_loads:
        c.wait()

    squares = jnp.zeros((8, 128), F32)
    for k in range(6):
        g = at(k, gg, gd)[...].astype(F32)
        g = g * g
        part = g[0:8]
        for i in range(1, g.shape[0] // 8):
            part = part + g[8 * i : 8 * i + 8]
        for i in range(part.shape[1] // 128):
            squares = squares + part[:, 128 * i : 128 * i + 128]
    sums.at[dp][...] = squares
    pl.semaphore_wait(barrier, 15)

    def sum_copy(off):
        return remote(sums.at[dp], sums.at[dp], sum_send.at[off], sum_recv.at[off], rep, (dp + off) % 16)

    for off in range(1, 16):
        sum_copy(off).start()
    for c in loads:
        c.wait()
    for off in range(1, 16):
        sum_copy(off).wait_recv()
    mean = jnp.sum(sums[...]) / count
    factor = jnp.minimum(1.0, 0.5 * lax.rsqrt(jnp.full((8, 128), mean + 1e-30, F32)))[0:1, 0:1]

    def block(k, who):
        which, layer_ = items[k]
        return w_out[which].at[layer_, who]

    def gather_copy(k, s, who, src=None):
        src = block(k, who) if src is None else src
        return remote(src, block(k, who), ag_send.at[k, s], ag_recv.at[k, s], rep, to)

    def d2d_copy(k, s, who, src=None):
        src = block(k, who) if src is None else src
        return remote(src, block(k, who), d2d_send.at[k, s], d2d_recv.at[k, s], rep, partner)

    stores = []
    for k, (which, layer_) in enumerate(items):
        g = at(k, gg, gd)[...].astype(F32) * factor
        mk, vk, wk = at(k, mg, md), at(k, vg, vd), at(k, wg, wd)
        new_m = 0.9 * mk[...] + 0.1 * g
        new_v = 0.95 * vk[...] + 0.05 * g * g
        wide = wk[...].astype(F32)
        wk[...] = (wide - 0.02 * (new_m * lax.rsqrt(new_v + 1e-8) + 0.1 * wide)).astype(BF16)
        mk[...] = new_m
        vk[...] = new_v
        gather_copy(k, 0, dp, wk).start()
        d2d_copy(k, 0, dp, wk).start()
        for n, (src, dst) in enumerate((
            (wk, block(k, dp)), (mk, m_out[which].at[layer_]), (vk, v_out[which].at[layer_]))):
            c = pltpu.make_async_copy(src, dst, store_sem.at[k, n])
            c.start()
            stores.append(c)

    def source(s):
        return 2 * ring((place - way * (1 + s) + 16) % 8) + core

    def gather(s, z):
        for k in range(6):
            who = source(s)
            gather_copy(k, s, who).wait_recv()
            gather_copy(k, s + 1, who).start()
            d2d_copy(k, s + 1, who).start()
        return z

    lax.fori_loop(0, 6, gather, 0)
    for k in range(6):
        who = source(6)
        gather_copy(k, 6, who).wait_recv()
        d2d_copy(k, 7, who).start()

    for c in stores:
        c.wait()
    for off in range(1, 16):
        sum_copy(off).wait_send()

    def drain(s, z):
        for k in range(6):
            gather_copy(k, s, dp).wait_send()
            d2d_copy(k, s, dp).wait_send()
            d2d_copy(k, s, dp).wait_recv()
        return z

    lax.fori_loop(0, 7, drain, 0)
    for k in range(6):
        d2d_copy(k, 7, dp).wait_send()
        d2d_copy(k, 7, dp).wait_recv()


def update(count, gg, gd, weights, m, v):
    G, S = (2, 2, 40, FF), (2, 160, D)
    any_ = pl.BlockSpec(memory_space=pl.ANY)
    dma, vmem = pltpu.SemaphoreType.DMA, pltpu.VMEM
    return pl.pallas_call(
        functools.partial(update_kernel, count),
        out_shape=[
            *(jax.ShapeDtypeStruct(t.shape, BF16) for t in weights),
            *(jax.ShapeDtypeStruct(t.shape, F32) for t in (*m, *v)),
        ],
        in_specs=[pl.BlockSpec(memory_space=pltpu.HBM)] * 11,
        out_specs=[any_] * 9,
        scratch_shapes=[
            vmem(G, BF16), vmem(S, BF16), vmem(G, F32), vmem(S, F32), vmem(G, F32), vmem(S, F32), vmem(G, BF16), vmem(S, BF16),
            vmem((16, 8, 128), F32),
            dma((2,)), dma((6, 3)), dma((16,)), dma((16,)),
            dma((6, 7)), dma((6, 7)), dma((6, 8)), dma((6, 8)), dma((6, 3)),
        ],
        compiler_params=pltpu.CompilerParams(
            collective_id=0, has_side_effects=True, vmem_limit_bytes=16 * 1024 * 1024),
    )(*(pltpu.with_memory_space_constraint(t, pltpu.HBM) for t in (gg, gd, *weights, *m, *v)))


def out_kernel(n, *refs):
    copies = [pltpu.make_async_copy(refs[i], refs[n + i], refs[2 * n].at[i]) for i in range(n)]
    for c in copies:
        c.start()
    for c in copies:
        c.wait()


def put_out(arrays):
    n = len(arrays)
    return pl.pallas_call(
        functools.partial(out_kernel, n),
        out_shape=[jax.ShapeDtypeStruct(t.shape, t.dtype) for t in arrays],
        in_specs=[pl.BlockSpec(memory_space=pl.ANY)] * n,
        out_specs=[pl.BlockSpec(memory_space=pltpu.HBM)] * n,
        scratch_shapes=[pltpu.SemaphoreType.DMA((n,))],
        compiler_params=pltpu.CompilerParams(vmem_limit_bytes=1024 * 1024),
    )(*arrays)


def solution(mesh):
    def body(x, dy, *arrays):
        weights, m, v = (arrays[i : i + 3] for i in (0, 3, 6))
        gg, gd = grads(x[0], dy[0], *weights)
        blocks = [w.reshape(2, 16, -1, w.shape[-1]) for w in weights]
        count = float(sum(w.size for w in weights))
        out = put_out(update(count, gg, gd, blocks, m, v))
        return (*(o.reshape(w.shape) for o, w in zip(out[:3], weights)), *out[3:])

    whole, rows = P(None, None, None), P(None, "dp", None)
    return jax.shard_map(
        body,
        mesh=mesh,
        in_specs=(P(("rep", "dp"), None, None),) * 2 + (whole,) * 3 + (rows,) * 6,
        out_specs=(P("rep", None, None),) * 3 + (P("rep", "dp", None),) * 6,
        check_vma=False,
    )
```
